32 devices in a mesh: comp: 2 (over core), aa: 2 (over y), ba: 8 (over z, x).
Axes of the slice: x: 2, y: 2, z: 4, core: 2. Of those that a mesh axis runs over, the one named last changes fastest.
Arguments:
- legendre: bfloat16 [640, 8, 1280], P('aa'), may hold values from -0.15625 to 0.15625
- coefficients: bfloat16 [2, 640, 2, 64, 1280], P('comp', 'aa', None, 'ba'), may hold values from -0.1796875 to 0.1796875
- cycle_points: int32 [8], replicated, may hold values from 1024 to 4096, as said below
- spectra: float32 [32, 256, 1296], P('aa', 'ba', 'comp'), may hold values from 0.05 to 2
- sea_mask: int32 [32, 256], P('aa', 'ba'), may hold values 0 or 1
- wind_column: int32 [32, 256], P('aa'), may hold values from 0 to 4095, as said below
- roughness_source: int32 [8, 4096], P('aa', 'ba'), may hold values from 0 to 4095, as said below
Outputs:
- grid_winds: bfloat16 [2, 8, 64, 4096], P('comp', 'aa', None, 'ba')
- wave_spectra: float32 [32, 256, 1296], P('aa', 'ba', 'comp')
- charnock: float32 [8, 4096], P('aa', 'ba')
The draws below stay inside these ranges and needn't reach their ends.
Inputs may be any that keep to these rules, and one draw needn't show every extreme that they name: `cycle_points`: at least a quarter of 4096; one cycle has exactly 4096 points. `wind_column`: each value is below the point count of cycle row // 4. `roughness_source`: the row within the band is one of the 4 rows (l mod 4) * 4 onward.
All inputs are finite; a program needn't handle non-finite values. No bound on the sum of `sea_mask` on one device may be relied on, other than what follows from the above.
Results may differ from the reference program's by a relative error of at most 0.0046.
The reference program's roundings to bfloat16 on the way count: a program that leaves them out, or rounds other values in their place, can miss the bound.
Values may be sent and summed in bfloat16 or wider, within the bound.
No kernel may reach another device: no remote copies, remote signals or barrier semaphores. Data moves between devices by JAX's collectives and lax.ppermute only.
A program may use at most 64 MiB of HBM per device.

```python
import math
import jax
import jax.numpy as jnp
from jax import lax

MW = 640
NT = 1280
LEV = 64
LON = 4096
LAT_DEV = 4
CYCLE_ROWS = 4
NDIR = 36
NFREQ = 36
WSTEPS = 2
LAT = 8
WLAT_DEV = 16
WLAT = 32
WLON = 256
BINS = 1296
N_AA = 2


def point_counts(key):
    subkey = jax.random.fold_in(key, 17)
    drawn = jax.random.randint(jax.random.fold_in(subkey, 1), (LAT,), LON // 4, LON + 1)
    fullest = jax.random.randint(jax.random.fold_in(subkey, 2), (), 0, LAT)
    return jnp.where(jnp.arange(LAT) == fullest, LON, drawn).astype(jnp.int32)


def draw_cycle_points(key, part):
    return point_counts(key)


def draw_wind_column(key, part):
    counts = point_counts(key)
    row_cycles = jnp.arange(WLAT) // CYCLE_ROWS
    per_row = counts[row_cycles][:, None]
    columns = jnp.arange(WLON)[None, :]
    centred = (2 * columns + 1) * per_row // (2 * WLON)
    jitter = jax.random.randint(jax.random.fold_in(key, 23), (WLAT, WLON), -2, 3)
    return ((centred + jitter + per_row) % per_row).astype(jnp.int32)


def draw_roughness_source(key, part):
    counts = point_counts(key)[:, None]
    cycles = jnp.arange(LAT)[:, None]
    slot_index = jnp.arange(LON)[None, :]
    row_pick = cycles % LAT_DEV * CYCLE_ROWS + jax.random.randint(jax.random.fold_in(key, 29), (LAT, LON), 0, CYCLE_ROWS)
    column = (2 * slot_index + 1) * WLON // (2 * counts)
    column = column + jax.random.randint(jax.random.fold_in(key, 31), (LAT, LON), -1, 2)
    column = jnp.clip(column, 0, WLON - 1)
    return (row_pick * WLON + column).astype(jnp.int32)


def place_ends(array, own_key, smallest, top_value):
    spot = [jax.random.randint(jax.random.fold_in(own_key, axis), (), 0, length) for axis, length in enumerate(array.shape)]
    widest = array.shape.index(max(array.shape))
    next_to = spot[:widest] + [(spot[widest] + 1) % array.shape[widest]] + spot[widest + 1:]
    return array.at[tuple(spot)].set(smallest).at[tuple(next_to)].set(top_value)


def levels(stream_key, dims, cuts, low, largest):
    loudness = 1.0
    for position, parts in cuts:
        heights = jax.random.uniform(jax.random.fold_in(jax.random.fold_in(stream_key, 6), position), (parts,), jnp.float32, low / len(cuts), largest / len(cuts))
        loudness = loudness * jnp.repeat(jnp.exp(heights), dims[position] // parts).reshape((-1,) + (1,) * (len(dims) - 1 - position))
    return loudness


def bell_draw(stream_key, extent, spread, most, split=(), kind=jnp.bfloat16):
    array = spread * jax.random.normal(stream_key, extent, jnp.float32)
    if split:
        array = array * levels(stream_key, extent, split, -0.22, 0.18)
    return jnp.clip(array, -most, most).astype(kind)


def setup_inputs(seed: int = 0) -> dict:
    seeds = jax.random.split(jax.random.key(seed), 8)
    return {
        "legendre": bell_draw(seeds[0], (MW, LAT, NT), NT ** -0.5, 0.15625, ((0, 2),)),
        "coefficients": bell_draw(seeds[1], (2, MW, 2, LEV, NT), 0.03, 0.1796875, ((0, 2), (1, 2), (3, 8))),
        "cycle_points": draw_cycle_points(jax.random.fold_in(seeds[7], 71), 0),
        "spectra": jnp.clip(jnp.exp(math.log(2.0) - 3.6888794 * jax.random.uniform(seeds[3], (WLAT, WLON, BINS), jnp.float32) ** levels(seeds[3], (WLAT, WLON, BINS), ((0, 2), (1, 8), (2, 2)), -0.2, 0.2)), 0.05, 2.0),
        "sea_mask": place_ends((jax.random.randint(seeds[4], (WLAT, WLON), 0, 3) < 2).astype(jnp.int32), jax.random.fold_in(seeds[4], 1), 0, 1),
        "wind_column": draw_wind_column(jax.random.fold_in(seeds[7], 71), 0),
        "roughness_source": draw_roughness_source(jax.random.fold_in(seeds[7], 71), 0),
    }


two_pi = 2.0 * math.pi
gravity = 9.81
base_freq = 0.04177
courant = 0.45
wind_scale = 10.0
growth = 0.05
dissipation = 0.5
energy_ref = 8.0
mid_freq = 0.2
stress_coef = 0.03
drag_coef = 0.0012
stress_floor = 0.02

def cycle_tables(cycle_counts, slot_index, wave_count):
    orders = jnp.arange(wave_count, dtype=jnp.int32)
    remain = orders[None, :, None] * slot_index[None, None, :] % cycle_counts[:, None, None]
    phases = two_pi * remain.astype(jnp.float32) / cycle_counts.astype(jnp.float32)[:, None, None]
    weight = jnp.where(orders == 0, 1.0, 2.0).astype(jnp.float32)[None, :, None]
    active = slot_index[None, None, :] < cycle_counts[:, None, None]
    cosine_part = jnp.where(active, weight * jnp.cos(phases), 0.0)
    sine_part = jnp.where(active, -weight * jnp.sin(phases), 0.0)
    return jnp.stack([cosine_part, sine_part], axis=1).astype(jnp.bfloat16)

def bin_constants(directions, freq_index):
    heading = two_pi * (directions.astype(jnp.float32) + 0.5) / NDIR
    freq_step = 35.0 / (NFREQ - 1)
    period_ratio = jnp.exp(-math.log(1.1) * freq_step * freq_index.astype(jnp.float32))
    frequency = base_freq / period_ratio
    cosine_dir = jnp.cos(heading)
    sine_dir = jnp.sin(heading)
    drift_east = courant * period_ratio * cosine_dir
    drift_north = courant * period_ratio * sine_dir
    inverse_speed = two_pi * frequency / gravity
    bin_width = 0.1 * frequency * (two_pi / NDIR)
    return (frequency, cosine_dir, sine_dir, drift_east, drift_north, inverse_speed, bin_width)

def advect(padded, drift_east, drift_north):
    centre = padded[1:-1, 1:-1]
    western = padded[1:-1, :-2]
    eastern = padded[1:-1, 2:]
    southern = padded[:-2, 1:-1]
    northern = padded[2:, 1:-1]
    east_pos = jnp.maximum(drift_east, 0.0)
    east_neg = jnp.minimum(drift_east, 0.0)
    north_pos = jnp.maximum(drift_north, 0.0)
    north_neg = jnp.minimum(drift_north, 0.0)
    return centre - east_pos * (centre - western) - east_neg * (eastern - centre) - north_pos * (centre - southern) - north_neg * (northern - centre)

def wind_terms(density, east_wind, north_wind, cosine_dir, sine_dir, inverse_speed, bin_width):
    alignment = (east_wind[..., None] * cosine_dir + north_wind[..., None] * sine_dir) * inverse_speed
    wind_gain = growth * jnp.maximum(alignment - 1.0, 0.0)
    energy_part = lax.optimization_barrier(jnp.sum(density * bin_width, axis=-1))
    stress_part = lax.optimization_barrier(jnp.sum(wind_gain * density * alignment * bin_width, axis=-1))
    return (wind_gain, energy_part, stress_part)

def finish(density, wind_gain, energy, stress, east_wind, north_wind, frequency):
    decay_rate = dissipation * (frequency / mid_freq) * jnp.square(energy / energy_ref)[..., None]
    spectra_after = density * (1.0 + wind_gain) / (1.0 + decay_rate)
    air_stress = drag_coef * (east_wind * east_wind + north_wind * north_wind) + stress_floor
    roughness = jnp.sqrt(1.0 + stress_coef * stress / air_stress)
    return (spectra_after, roughness)

def reference(legendre, coefficients, cycle_points, spectra, sea_mask, wind_column, roughness_source):
    degrees = jnp.arange(NT, dtype=jnp.int32)

    def legendre_order(order_index):
        legendre_row = lax.dynamic_index_in_dim(legendre, order_index, 0, keepdims=False)
        legendre_row = jnp.where(degrees[None, :] >= order_index, legendre_row, jnp.zeros((), jnp.bfloat16))
        coeff_block = lax.dynamic_index_in_dim(coefficients, order_index, 1, keepdims=False)
        return jnp.einsum('ln,spcn->lspc', legendre_row.astype(jnp.float32), coeff_block.astype(jnp.float32))
    fourier = lax.map(legendre_order, jnp.arange(MW, dtype=jnp.int32)).astype(jnp.bfloat16)
    slot_index = jnp.arange(LON, dtype=jnp.int32)

    def synthesize(cycle_index):
        cycle_count = lax.dynamic_slice_in_dim(cycle_points, cycle_index, 1)
        tables = cycle_tables(cycle_count, slot_index, MW)[0]
        cycle_block = lax.dynamic_index_in_dim(fourier, cycle_index, 1, keepdims=False)
        grid_field = jnp.einsum('mspc,pmk->sck', cycle_block.astype(jnp.float32), tables.astype(jnp.float32))
        return grid_field.astype(jnp.bfloat16)
    grid_field = lax.map(synthesize, jnp.arange(LAT, dtype=jnp.int32))
    grid_winds = jnp.transpose(grid_field, (1, 0, 2, 3))
    bin_index = jnp.arange(NDIR * NFREQ, dtype=jnp.int32)
    frequency, cosine_dir, sine_dir, drift_east, drift_north, inverse_speed, bin_width = bin_constants(bin_index // NFREQ, bin_index % NFREQ)
    sea_float = sea_mask.astype(jnp.float32)[:, :, None]
    density = spectra * sea_float
    for substep in range(WSTEPS):
        padded = jnp.pad(density, ((1, 1), (1, 1), (0, 0)))
        density = advect(padded, drift_east, drift_north) * sea_float
    lowest = grid_winds[:, :, 0, :].astype(jnp.float32)
    repeated = jnp.repeat(lowest, CYCLE_ROWS, axis=1)
    picked = jnp.take_along_axis(repeated, jnp.broadcast_to(wind_column[None], (2, WLAT, WLON)), axis=2)
    east_wind = wind_scale * picked[0]
    north_wind = wind_scale * picked[1]
    wind_gain, energy, stress = wind_terms(density, east_wind, north_wind, cosine_dir, sine_dir, inverse_speed, bin_width)
    wave_spectra, roughness = finish(density, wind_gain, energy, stress, east_wind, north_wind, frequency)
    band_ratio = roughness.reshape(N_AA, WLAT_DEV * WLON)
    per_cycle = jnp.repeat(band_ratio, LAT_DEV, axis=0)
    values = jnp.take_along_axis(per_cycle, roughness_source, axis=1)
    active = slot_index[None, :] < cycle_points[:, None]
    charnock = jnp.where(active, values, 0.0)
    return (grid_winds, wave_spectra, charnock)
```

```python
import functools
import math

import jax
import jax.numpy as jnp
import numpy as np
from jax import lax
from jax.experimental import pallas as pl
from jax.experimental.pallas import tpu as pltpu
from jax.sharding import PartitionSpec as P

LON = 4096
NDIR = 36
NFREQ = 36
LANES = 128
PAD = 8

two_pi = 2.0 * math.pi
gravity = 9.81
base_freq = 0.04177
courant = 0.45
wind_scale = 10.0
growth = 0.05
dissipation = 0.5
energy_ref = 8.0
mid_freq = 0.2
stress_coef = 0.03
drag_coef = 0.0012
stress_floor = 0.02

bf16 = jnp.bfloat16
f32 = jnp.float32
SMEM_SPEC = pl.BlockSpec(memory_space=pltpu.SMEM)


def vmem_spec():
    return pl.BlockSpec(memory_space=pltpu.VMEM)


def params(parallel=1):
    return pltpu.CompilerParams(
        dimension_semantics=("arbitrary",) * parallel, vmem_limit_bytes=48 * 1024 * 1024
    )


def cost(flops, nbytes):
    return pl.CostEstimate(flops=flops, bytes_accessed=nbytes, transcendentals=0)


def legendre_kernel(
    shape, where_ref, leg_ref, coef_ref, out_ref, held
):
    n_aa, waves_local, cycles, pc, group, per_step, wave_lanes = shape
    step = pl.program_id(0)
    band = where_ref[0]
    band_cycles = cycles // n_aa
    per_block = LANES // group

    @pl.when(step == 0)
    def _():
        held[...] = jnp.zeros_like(held)

    lane = lax.broadcasted_iota(jnp.int32, (pc, LANES), 1)
    row_wave = lax.broadcasted_iota(jnp.int32, (group * cycles, wave_lanes), 0) // cycles
    degree = lax.broadcasted_iota(jnp.int32, (group * cycles, wave_lanes), 1)
    contract = (((1,), (1,)), ((), ()))
    for part in range(per_step):
        index = step * per_step + part
        leg_rows = pl.ds(part * group * cycles, group * cycles)
        coef_rows = pl.ds(part * group * pc, group * pc)
        first = band * waves_local + index * group
        low = leg_ref[leg_rows, :wave_lanes].astype(f32)
        low = jnp.where(degree >= row_wave + first, low, 0.0).astype(bf16)
        full = lax.dot_general(
            coef_ref[coef_rows, :wave_lanes], low, contract, preferred_element_type=f32
        ) + lax.dot_general(
            coef_ref[coef_rows, wave_lanes:],
            leg_ref[leg_rows, wave_lanes:],
            contract,
            preferred_element_type=f32,
        )
        own = jnp.zeros((pc, LANES), f32)
        for wave in range(group):
            own = own + jnp.where(lane // cycles == wave, full[wave * pc : (wave + 1) * pc], 0.0)
        block = index // per_block
        here = lane // group == index % per_block
        for cycle in range(cycles):
            source = (lane % group) * cycles + cycle
            piece = jnp.take_along_axis(own, source, axis=1)
            held[block, cycle] = jnp.where(here, piece, held[block, cycle])

    @pl.when(step == pl.num_programs(0) - 1)
    def _():
        for shift in range(n_aa):
            target = lax.rem(band + shift, n_aa)
            for cycle in range(band_cycles):
                for block in range(held.shape[0]):
                    out_ref[shift, cycle, :, block * LANES : (block + 1) * LANES] = held[
                        block, target * band_cycles + cycle
                    ].astype(bf16)


def legendre_sums(legendre, coefficients, band_index, n_aa):
    waves_local, cycles, degrees = legendre.shape
    pc = coefficients.shape[2] * coefficients.shape[3]
    group = LANES // cycles
    per_step = 32 // group if waves_local % 32 == 0 else 16 // group
    rows = group * per_step
    steps = waves_local // rows
    blocks = -(-waves_local // LANES)
    wave_lanes = -(-waves_local * n_aa // LANES) * LANES
    shape = (n_aa, waves_local, cycles, pc, group, per_step, wave_lanes)
    return pl.pallas_call(
        functools.partial(legendre_kernel, shape),
        grid=(steps,),
        in_specs=[
            SMEM_SPEC,
            pl.BlockSpec((rows * cycles, degrees), lambda i: (i, 0)),
            pl.BlockSpec((rows * pc, degrees), lambda i: (i, 0)),
        ],
        out_specs=pl.BlockSpec(
            (n_aa, cycles // n_aa, pc, blocks * LANES), lambda i: (0, 0, 0, 0)
        ),
        out_shape=jax.ShapeDtypeStruct((n_aa, cycles // n_aa, pc, blocks * LANES), bf16),
        scratch_shapes=[pltpu.VMEM((blocks, cycles, pc, LANES), f32)],
        compiler_params=params(),
        cost_estimate=cost(7_000_000_000, 20_000_000),
        name="legendre",
    )(
        band_index,
        legendre.reshape(waves_local * cycles, degrees),
        coefficients.reshape(waves_local * pc, degrees),
    )


def sine_cosine(wave, slot, points, inverse):
    product = wave * slot
    remain = product - jnp.floor(product * inverse + 0.5) * points
    turn = remain / points
    quarter = jnp.floor(4.0 * turn + 0.5)
    angle = (turn - 0.25 * quarter) * two_pi
    square = angle * angle
    sine = angle * (
        1.0
        + square
        * (-1.0 / 6.0 + square * (1.0 / 120.0 + square * (-1.0 / 5040.0 + square / 362880.0)))
    )
    cosine = 1.0 + square * (
        -0.5 + square * (1.0 / 24.0 + square * (-1.0 / 720.0 + square / 40320.0))
    )
    side = jnp.abs(quarter) == 1.0
    back = jnp.abs(quarter) == 2.0
    cosine_out = jnp.where(side, -quarter * sine, jnp.where(back, -cosine, cosine))
    sine_out = jnp.where(side, quarter * cosine, jnp.where(back, -sine, sine))
    return sine_out, cosine_out


def table_kernel(shape, where_ref, count_ref, slot_ref, out_ref, coarse):
    n_aa, waves_local, fine_rows = shape
    coarse_local = waves_local // fine_rows
    coarse_rows = coarse.shape[1]
    band = where_ref[0]
    cycle = pl.program_id(0)
    points = count_ref[cycle].astype(f32)
    slot = slot_ref[0]
    width = slot.shape[1]
    points_row = jnp.full((1, width), points, f32)
    inverse = 1.0 / points_row
    active = slot < points_row
    fine = lax.broadcasted_iota(jnp.int32, (fine_rows, width), 0).astype(f32)
    sine_fine, cosine_fine = sine_cosine(fine, slot, points_row, inverse)
    row = lax.broadcasted_iota(jnp.int32, (coarse_rows, width), 0)
    wave = jnp.zeros((coarse_rows, width), jnp.int32)
    for shift in range(n_aa):
        first = lax.rem(band - shift + n_aa, n_aa) * waves_local
        inside = (row >= shift * coarse_local) & (row < (shift + 1) * coarse_local)
        wave = jnp.where(inside, first + (row - shift * coarse_local) * fine_rows, wave)
    sine_coarse, cosine_coarse = sine_cosine(wave.astype(f32), slot, points_row, inverse)
    coarse[0] = jnp.where(active, 2.0 * cosine_coarse, 0.0)
    coarse[1] = jnp.where(active, 2.0 * sine_coarse, 0.0)
    for shift in range(n_aa):
        first = lax.rem(band - shift + n_aa, n_aa) * waves_local
        for step in range(coarse_local):
            at = shift * coarse_local + step
            cosine_at = coarse[0, at : at + 1, :]
            sine_at = coarse[1, at : at + 1, :]
            cosine_part = cosine_at * cosine_fine - sine_at * sine_fine
            sine_part = -(sine_at * cosine_fine + cosine_at * sine_fine)
            if step == 0:
                weight = jnp.where(fine + first.astype(f32) == 0.0, 0.5, 1.0)
                cosine_part = cosine_part * weight
                sine_part = sine_part * weight
            rows = slice(at * fine_rows, (at + 1) * fine_rows)
            out_ref[0, 0, rows, :] = cosine_part.astype(bf16)
            out_ref[0, 1, rows, :] = sine_part.astype(bf16)


def tables(slots, counts, band_index, n_aa, waves_local, name):
    cycles, width = slots.shape
    fine_rows = 32 if waves_local % 32 == 0 else 16
    waves = n_aa * waves_local
    coarse_rows = -(-(waves // fine_rows) // 8) * 8
    return pl.pallas_call(
        functools.partial(table_kernel, (n_aa, waves_local, fine_rows)),
        grid=(cycles,),
        in_specs=[
            SMEM_SPEC,
            SMEM_SPEC,
            pl.BlockSpec((1, 1, width), lambda i: (i, 0, 0)),
        ],
        out_specs=pl.BlockSpec((1, 2, waves, width), lambda i: (i, 0, 0, 0)),
        out_shape=jax.ShapeDtypeStruct((cycles, 2, waves, width), bf16),
        scratch_shapes=[pltpu.VMEM((2, coarse_rows, width), f32)],
        compiler_params=params(),
        cost_estimate=cost(cycles * waves * width * 500, cycles * waves * width * 4),
        name=name,
    )(band_index, counts, slots.reshape(cycles, 1, width))


def stack_rows(pieces):
    if pieces[0].shape[0] % 16 == 0:
        return jnp.concatenate(pieces, axis=0)
    return jnp.concatenate([piece.astype(f32) for piece in pieces], axis=0).astype(bf16)


def synthesis_kernel(shape, where_ref, *refs):
    n_aa, waves_local, n_out, n_in = shape
    fourier, (table_ref, out_ref) = refs[:n_in], refs[n_in:]
    column = where_ref[1]
    levels = out_ref.shape[2]
    pc = fourier[0].shape[3]
    cosine_sum = None
    sine_sum = None
    for shift in range(n_aa):
        left = stack_rows(
            [
                fourier[inner][outer, shift, 0, :, :waves_local]
                for inner in range(n_in)
                for outer in range(n_out)
            ]
        )
        rows = slice(shift * waves_local, (shift + 1) * waves_local)
        cosine_part = jnp.dot(left, table_ref[0, 0, rows, :], preferred_element_type=f32)
        sine_part = jnp.dot(left, table_ref[0, 1, rows, :], preferred_element_type=f32)
        cosine_sum = cosine_part if cosine_sum is None else cosine_sum + cosine_part
        sine_sum = sine_part if sine_sum is None else sine_sum + sine_part
    for inner in range(n_in):
        for outer in range(n_out):
            at = (inner * n_out + outer) * pc
            value = cosine_sum[at : at + levels] + sine_sum[at + levels : at + pc]
            source = jnp.bitwise_xor(column, outer * n_in + inner)
            out_ref[0, source] = value.astype(bf16)


def synthesis(fourier, table, where, n_aa, waves_local, n_in):
    n_out, _, cycles, pc, lanes = fourier[0].shape
    width = table.shape[3]
    levels = pc // 2
    n_ba = n_out * n_in
    block = pl.BlockSpec((n_out, n_aa, 1, pc, lanes), lambda i: (0, 0, i, 0, 0))
    return pl.pallas_call(
        functools.partial(synthesis_kernel, (n_aa, waves_local, n_out, n_in)),
        grid=(cycles,),
        in_specs=[SMEM_SPEC]
        + [block] * n_in
        + [pl.BlockSpec((1, 2, table.shape[2], width), lambda i: (i, 0, 0, 0))],
        out_specs=pl.BlockSpec((1, n_ba, levels, width), lambda i: (i, 0, 0, 0)),
        out_shape=jax.ShapeDtypeStruct((cycles, n_ba, levels, width), bf16),
        compiler_params=params(),
        cost_estimate=cost(1_500_000_000, 6_000_000),
        name="synthesis",
    )(where, *fourier, table)


def pick_kernel(shape, where_ref, *refs):
    n_aa, waves_local, n_out, n_in = shape
    fourier, (table_ref, out_ref) = refs[:n_in], refs[n_in:]
    column = where_ref[1]
    inner_at = lax.rem(column, n_in)
    outer_at = column // n_in
    cycles = out_ref.shape[0]
    pc = fourier[0].shape[3]
    levels = pc // 2
    for cycle in range(cycles):
        total = None
        for shift in range(n_aa):
            left = fourier[0][outer_at, shift, cycle].astype(f32)
            for inner in range(1, n_in):
                other = fourier[inner][outer_at, shift, cycle].astype(f32)
                left = jnp.where(inner_at == inner, other, left)
            left = left[:, :waves_local].astype(bf16)
            rows = slice(shift * waves_local, (shift + 1) * waves_local)
            cosine_part = jnp.dot(left, table_ref[cycle, 0, rows, :], preferred_element_type=f32)
            sine_part = jnp.dot(left, table_ref[cycle, 1, rows, :], preferred_element_type=f32)
            part = cosine_part[0:1] + sine_part[levels : levels + 1]
            total = part if total is None else total + part
        out_ref[cycle : cycle + 1, :] = wind_scale * total.astype(bf16).astype(f32)


def pick_winds(fourier, table, where, n_aa, waves_local, n_in):
    n_out, _, cycles, pc, lanes = fourier[0].shape
    width = table.shape[3]
    return pl.pallas_call(
        functools.partial(pick_kernel, (n_aa, waves_local, n_out, n_in)),
        in_specs=[SMEM_SPEC] + [vmem_spec()] * (n_in + 1),
        out_specs=vmem_spec(),
        out_shape=jax.ShapeDtypeStruct((cycles, width), f32),
        compiler_params=params(0),
        cost_estimate=cost(500_000_000, 2_000_000),
        name="pick",
    )(where, *fourier, table)


def bin_table(parts):
    bins = np.arange(NDIR * NFREQ)
    directions, freq_index = bins // NFREQ, bins % NFREQ
    heading = two_pi * (directions + 0.5) / NDIR
    period_ratio = np.exp(-math.log(1.1) * (35.0 / (NFREQ - 1)) * freq_index)
    frequency = base_freq / period_ratio
    drift_east = courant * period_ratio * np.cos(heading)
    drift_north = courant * period_ratio * np.sin(heading)
    inverse_speed = two_pi * frequency / gravity
    bin_width = 0.1 * frequency * (two_pi / NDIR)
    east_pos, east_neg = np.maximum(drift_east, 0.0), -np.minimum(drift_east, 0.0)
    north_pos, north_neg = np.maximum(drift_north, 0.0), -np.minimum(drift_north, 0.0)
    rows = [
        1.0 - east_pos - east_neg - north_pos - north_neg,
        east_pos,
        east_neg,
        north_pos,
        north_neg,
        np.cos(heading) * inverse_speed,
        np.sin(heading) * inverse_speed,
        bin_width,
        dissipation * (frequency / mid_freq),
    ]
    rows += [np.zeros_like(frequency)] * (16 - len(rows))
    table = np.stack(rows).astype(np.float32).reshape(16, parts, -1)
    return np.ascontiguousarray(table.transpose(1, 0, 2))


def advect_kernel(
    bins_ref, spectra_ref, mask_ref, low_ref, high_ref, west_ref, east_ref, out_ref, first, second
):
    rows, columns, bins = spectra_ref.shape
    wide = columns + 2 * PAD
    mask = jnp.transpose(mask_ref[...])
    lane = lax.broadcasted_iota(jnp.int32, mask.shape, 1)

    def column_mask(row):
        return jnp.sum(jnp.where(lane == row, mask, 0.0), axis=1, keepdims=True)[:columns]

    edge = jnp.zeros((PAD, bins), f32)
    for row in range(rows + 4):
        first[row, 0:PAD] = edge
        first[row, PAD + columns :] = edge
    masks = []
    for row in range(-2, rows + 2):
        if row < 0:
            block = low_ref[row + 2]
        elif row >= rows:
            block = high_ref[row - rows]
        else:
            own = column_mask(row)
            first[row + 2, PAD : PAD + columns] = spectra_ref[row] * own
            masks.append(own)
            continue
        first[row + 2, PAD : PAD + columns] = block[:, :bins]
        if row in (-1, rows):
            masks.append(block[:, bins : bins + 1])
    first[1 : rows + 3, PAD - 2 : PAD] = west_ref[:, :, :bins]
    first[1 : rows + 3, PAD + columns : PAD + columns + 2] = east_ref[:, :, :bins]
    keep, east_pos, east_neg = bins_ref[0:1], bins_ref[1:2], bins_ref[2:3]
    north_pos, north_neg = bins_ref[3:4], bins_ref[4:5]

    def update(source, at):
        centre = source[at]
        western = pltpu.roll(centre, 1, 0)
        eastern = pltpu.roll(centre, wide - 1, 0)
        return (
            keep * centre
            + east_pos * western
            + east_neg * eastern
            + north_pos * source[at - 1]
            + north_neg * source[at + 1]
        )

    for row in range(rows + 2):
        value = update(first, row + 1)
        second[row, 0:PAD] = value[0:PAD]
        second[row, PAD : PAD + columns] = value[PAD : PAD + columns] * masks[row]
        second[row, PAD + columns :] = value[PAD + columns :]
        second[row, PAD - 1 : PAD] = (
            value[PAD - 1 : PAD] * west_ref[row, 1:2, bins : bins + 1]
        )
        second[row, PAD + columns : PAD + columns + 1] = (
            value[PAD + columns : PAD + columns + 1] * east_ref[row, 0:1, bins : bins + 1]
        )
    for row in range(rows):
        value = update(second, row + 1)
        out_ref[row] = value[PAD : PAD + columns] * masks[row + 1]


def advect(bins, spectra, mask, low, high, west, east):
    rows, columns, count = spectra.shape
    wide = columns + 2 * PAD
    padded = jnp.pad(mask, ((0, LANES - rows), (0, LANES - columns)))
    return pl.pallas_call(
        advect_kernel,
        in_specs=[vmem_spec()] * 7,
        out_specs=vmem_spec(),
        out_shape=jax.ShapeDtypeStruct(spectra.shape, f32),
        scratch_shapes=[
            pltpu.VMEM((rows + 4, wide, count), f32),
            pltpu.VMEM((rows + 2, wide, count), f32),
        ],
        compiler_params=params(0),
        cost_estimate=cost(2_000_000_000, 4_000_000),
        name="advect",
    )(bins, spectra, padded, low, high, west, east)


def halo(spectra, mask):
    def packed(part, part_mask):
        return jnp.concatenate([part * part_mask[:, :, None], part_mask[:, :, None]], axis=2)

    def shifted(low_side, high_side, axis):
        count = lax.axis_size(axis)
        index = lax.axis_index(axis)
        if count == 2:
            sent = jnp.where(index == 0, high_side, low_side)
            got = lax.ppermute(sent, axis, [(0, 1), (1, 0)])
            return jnp.where(index == 1, got, 0.0), jnp.where(index == 0, got, 0.0)
        forward = [(i, i + 1) for i in range(count - 1)]
        backward = [(target, source) for source, target in forward]
        return lax.ppermute(high_side, axis, forward), lax.ppermute(low_side, axis, backward)

    low, high = shifted(
        packed(spectra[:2], mask[:2]), packed(spectra[-2:], mask[-2:]), "aa"
    )
    sides = []
    for cut in (slice(0, 2), slice(-2, None)):
        own = packed(spectra[:, cut], mask[:, cut])
        sides.append(jnp.concatenate([low[1:, cut], own, high[:1, cut]], axis=0))
    west, east = shifted(sides[0], sides[1], "ba")
    return low, high, west, east


def winds_of(where_ref, own_ref, other_ref):
    first_component = where_ref[2] == 0
    own, other = own_ref[...], other_ref[...]
    return jnp.where(first_component, own, other), jnp.where(first_component, other, own)


def as_columns(rows_by_lanes):
    rows = rows_by_lanes.shape[0]
    if rows % 8:
        rows_by_lanes = jnp.concatenate(
            [rows_by_lanes, jnp.zeros((8 - rows % 8, LANES), f32)], axis=0
        )
    return jnp.transpose(rows_by_lanes)


def stress_kernel(where_ref, bins_ref, density_ref, own_ref, other_ref, out_ref):
    cycles = own_ref.shape[0]
    rows, columns, bins = density_ref.shape
    cycle_rows = rows // cycles
    east, north = winds_of(where_ref, own_ref, other_ref)
    east, north = as_columns(east), as_columns(north)
    along_cos, along_sin, width = bins_ref[5:6], bins_ref[6:7], bins_ref[7:8]
    lane = lax.broadcasted_iota(jnp.int32, (LANES, LANES), 1)
    sums = jnp.zeros((LANES, LANES), f32)
    for cycle in range(cycles):
        density = density_ref[cycle * cycle_rows : (cycle + 1) * cycle_rows].reshape(LANES, bins)
        alignment = (
            east[:, cycle : cycle + 1] * along_cos + north[:, cycle : cycle + 1] * along_sin
        )
        weighted = density * width
        gain = growth * jnp.maximum(alignment - 1.0, 0.0)
        energy = jnp.sum(weighted, axis=1, keepdims=True)
        stress = jnp.sum(gain * alignment * weighted, axis=1, keepdims=True)
        sums = jnp.where(lane == cycle, stress, sums)
        sums = jnp.where(lane == cycles + cycle, energy, sums)
    out_ref[...] = jnp.transpose(sums)[: 2 * cycles]


def stress_sums(where, bins, density, own, other):
    cycles = own.shape[0]
    return pl.pallas_call(
        stress_kernel,
        in_specs=[SMEM_SPEC] + [vmem_spec()] * 4,
        out_specs=vmem_spec(),
        out_shape=jax.ShapeDtypeStruct((2 * cycles, LANES), f32),
        compiler_params=params(0),
        cost_estimate=cost(500_000_000, 2_000_000),
        name="stress",
    )(where, bins, density, own, other)


def spectra_kernel(where_ref, bins_ref, density_ref, own_ref, other_ref, energy_ref_, out_ref):
    cycles = own_ref.shape[0]
    rows, columns, bins = density_ref.shape
    cycle_rows = rows // cycles
    east, north = winds_of(where_ref, own_ref, other_ref)
    east, north = as_columns(east), as_columns(north)
    scaled = energy_ref_[...] * (1.0 / energy_ref)
    energy = as_columns(scaled * scaled)
    along_cos, along_sin, decay = bins_ref[5:6], bins_ref[6:7], bins_ref[8:9]
    for cycle in range(cycles):
        at = slice(cycle * cycle_rows, (cycle + 1) * cycle_rows)
        density = density_ref[at].reshape(LANES, bins)
        alignment = (
            east[:, cycle : cycle + 1] * along_cos + north[:, cycle : cycle + 1] * along_sin
        )
        gain = growth * jnp.maximum(alignment - 1.0, 0.0)
        value = density * (1.0 + gain) / (1.0 + decay * energy[:, cycle : cycle + 1])
        out_ref[at] = value.reshape(cycle_rows, columns, bins)


def final_spectra(where, bins, density, own, other, energy):
    return pl.pallas_call(
        spectra_kernel,
        in_specs=[SMEM_SPEC] + [vmem_spec()] * 5,
        out_specs=vmem_spec(),
        out_shape=jax.ShapeDtypeStruct(density.shape, f32),
        compiler_params=params(0),
        cost_estimate=cost(500_000_000, 3_000_000),
        name="spectra",
    )(where, bins, density, own, other, energy)


def charnock_kernel(
    shape, where_ref, count_ref, rough_ref, source_ref, out_ref
):
    columns_local, total_columns = shape
    column = where_ref[1]
    pieces, cycles, _ = rough_ref.shape
    width = source_ref.shape[1]
    cycle_rows = LANES // columns_local
    base = column * width
    row = lax.broadcasted_iota(jnp.int32, (cycles, LANES), 0)
    points = jnp.zeros((cycles, LANES), jnp.int32)
    for cycle in range(cycles):
        points = jnp.where(row == cycle, count_ref[cycle], points)
    lane = lax.broadcasted_iota(jnp.int32, (cycles, LANES), 1)
    for part in range(width // LANES):
        at = slice(part * LANES, (part + 1) * LANES)
        source = source_ref[:, at]
        band_row = source // total_columns
        source_column = source - band_row * total_columns
        owner = source_column // columns_local
        within = (band_row - row * cycle_rows) * columns_local + (
            source_column - owner * columns_local
        )
        within = jnp.clip(within, 0, LANES - 1)
        value = jnp.zeros((cycles, LANES), f32)
        for piece in range(pieces):
            found = jnp.take_along_axis(rough_ref[piece], within, axis=1)
            value = jnp.where(owner == jnp.bitwise_xor(column, piece), found, value)
        out_ref[:, at] = jnp.where(lane + (base + part * LANES) < points, value, 0.0)


def charnock_of(where, counts, pieces, source, columns_local):
    return pl.pallas_call(
        functools.partial(charnock_kernel, (columns_local, columns_local * pieces.shape[0])),
        in_specs=[SMEM_SPEC, SMEM_SPEC] + [vmem_spec()] * 2,
        out_specs=vmem_spec(),
        out_shape=jax.ShapeDtypeStruct(source.shape, f32),
        compiler_params=params(0),
        cost_estimate=cost(100_000_000, 100_000),
        name="charnock",
    )(where, counts, pieces, source)


def exchange(value, axis, distance):
    count = lax.axis_size(axis)
    return lax.ppermute(value, axis, [(i, i ^ distance) for i in range(count)])


def per_device(
    legendre, coefficients, cycle_points, spectra, sea_mask, wind_column, roughness_source
):
    n_aa, n_ba = lax.axis_size("aa"), lax.axis_size("ba")
    n_comp = lax.axis_size("comp")
    band_index = lax.axis_index("aa")
    column_index = lax.axis_index("ba")
    half_index = lax.axis_index("comp")
    where = jnp.stack([band_index, column_index, half_index]).astype(jnp.int32)
    waves_local, cycles_all, _ = legendre.shape
    cycles = cycles_all // n_aa
    rows_local, columns_local, _ = spectra.shape
    cycle_rows = rows_local // cycles
    n_in = 2
    n_out = n_ba // n_in
    slots_local = LON // n_ba
    counts = lax.dynamic_slice_in_dim(cycle_points, band_index * cycles, cycles)
    bins = lax.dynamic_index_in_dim(jnp.asarray(bin_table(n_comp)), half_index, 0, keepdims=False)

    fourier = legendre_sums(legendre, coefficients, where, n_aa)

    mask = sea_mask.astype(f32)
    low, high, west, east = halo(spectra, mask)
    density = advect(bins, spectra, mask, low, high, west, east)

    own_slots = column_index * slots_local + jnp.arange(slots_local, dtype=jnp.int32)
    own_slots = jnp.broadcast_to(own_slots[None].astype(f32), (cycles, slots_local))
    wind_slots = lax.dynamic_slice_in_dim(
        wind_column, column_index * columns_local, columns_local, 1
    )
    wind_slots = wind_slots.astype(f32).reshape(cycles, cycle_rows * columns_local)
    wind_table = tables(wind_slots, counts, where, n_aa, waves_local, "wind_tables")
    grid_table = tables(own_slots, counts, where, n_aa, waves_local, "grid_tables")

    parts = [fourier[0]]
    for shift in range(1, n_aa):
        pairs = [(i, (i + shift) % n_aa) for i in range(n_aa)]
        parts.append(lax.ppermute(fourier[shift], "aa", pairs))
    parts = jnp.stack(parts)
    outer = [parts] + [exchange(parts, "ba", n_in * k) for k in range(1, n_out)]
    outer = jnp.stack(outer)
    inner = [outer] + [exchange(outer, "ba", k) for k in range(1, n_in)]

    own = pick_winds(inner, wind_table, where, n_aa, waves_local, n_in)
    other = exchange(own, "comp", 1)
    sums = stress_sums(where, bins, density, own, other)
    sums = sums + exchange(sums, "comp", 1)
    air = drag_coef * (own * own + other * other) + stress_floor
    roughness = jnp.sqrt(1.0 + stress_coef * sums[:cycles] / air)
    pieces = roughness[None]
    distance = 1
    while distance < n_ba:
        pieces = jnp.concatenate([pieces, exchange(pieces, "ba", distance)], axis=0)
        distance *= 2
    wave_spectra = final_spectra(where, bins, density, own, other, sums[cycles:])
    grid_winds = synthesis(inner, grid_table, where, n_aa, waves_local, n_in)
    grid_winds = grid_winds.reshape(1, cycles, -1, slots_local)
    charnock = charnock_of(where, counts, pieces, roughness_source, columns_local)
    return (grid_winds, wave_spectra, charnock)


def solution(mesh):
    in_specs = (
        P("aa", None, None),
        P("comp", "aa", None, "ba", None),
        P(),
        P("aa", "ba", "comp"),
        P("aa", "ba"),
        P("aa", None),
        P("aa", "ba"),
    )
    out_specs = (P("comp", "aa", None, "ba"), P("aa", "ba", "comp"), P("aa", "ba"))
    return jax.shard_map(
        per_device, mesh=mesh, in_specs=in_specs, out_specs=out_specs, check_vma=False
    )
```

```python
import functools
import math

import jax
import jax.numpy as jnp
import numpy as np
from jax import lax
from jax.experimental import pallas as pl
from jax.experimental.pallas import tpu as pltpu
from jax.sharding import PartitionSpec as P


LON = 4096
NDIR = 36
NFREQ = 36
LANES = 128
PAD = 8

two_pi = 2.0 * math.pi
gravity = 9.81
base_freq = 0.04177
courant = 0.45
wind_scale = 10.0
growth = 0.05
dissipation = 0.5
energy_ref = 8.0
mid_freq = 0.2
stress_coef = 0.03
drag_coef = 0.0012
stress_floor = 0.02


bf16 = jnp.bfloat16
f32 = jnp.float32
SMEM_SPEC = pl.BlockSpec(memory_space=pltpu.SMEM)


def vmem_spec():
    return pl.BlockSpec(memory_space=pltpu.VMEM)


def params(grid_dims=1, mebibytes=16):
    return pltpu.CompilerParams(
        dimension_semantics=("arbitrary",) * grid_dims, vmem_limit_bytes=mebibytes * 1024 * 1024
    )


def cost(flops, nbytes):
    return pl.CostEstimate(flops=flops, bytes_accessed=nbytes, transcendentals=0)


def legendre_kernel(shape, where_ref, leg_hbm, coef_hbm, *refs):
    n_aa, waves_local, cycles, pc, group, per_step, wave_lanes = shape
    out_refs, (leg_all, coef_all, held, arrived) = refs[:n_aa], refs[n_aa:]
    steps = leg_all.shape[0]
    band = where_ref[0]
    band_cycles = cycles // n_aa
    per_block = LANES // group
    groups = waves_local // group

    def copies(step):
        return (
            pltpu.make_async_copy(leg_hbm.at[step], leg_all.at[step], arrived.at[0, step]),
            pltpu.make_async_copy(coef_hbm.at[step], coef_all.at[step], arrived.at[1, step]),
        )

    for step in range(steps):
        for copy in copies(step):
            copy.start()

    lane = lax.broadcasted_iota(jnp.int32, (pc, LANES), 1)
    row_wave = lax.broadcasted_iota(jnp.int32, (group * cycles, wave_lanes), 0) // cycles
    degree = lax.broadcasted_iota(jnp.int32, (group * cycles, wave_lanes), 1)
    ahead = degree - row_wave
    contract = (((1,), (1,)), ((), ()))

    def one_step(step, carry):
        for copy in copies(step):
            copy.wait()
        for part in range(per_step):
            index = step * per_step + part
            leg_rows = pl.ds(part * group * cycles, group * cycles)
            coef_rows = pl.ds(part * group * pc, group * pc)
            first = band * waves_local + index * group
            low = leg_all[step, leg_rows, :wave_lanes].astype(f32)
            low = jnp.where(ahead >= first, low, 0.0).astype(bf16)
            full = lax.dot_general(
                coef_all[step, coef_rows, :wave_lanes],
                low,
                contract,
                preferred_element_type=f32,
            ) + lax.dot_general(
                coef_all[step, coef_rows, wave_lanes:],
                leg_all[step, leg_rows, wave_lanes:],
                contract,
                preferred_element_type=f32,
            )
            own = full[:pc]
            for wave in range(1, group):
                own = jnp.where(lane // cycles == wave, full[wave * pc : (wave + 1) * pc], own)
            held[index] = own
        return carry

    lax.fori_loop(0, steps, one_step, 0)

    for shift in range(n_aa):
        target = lax.rem(band + shift, n_aa) * band_cycles
        for cycle in range(band_cycles):
            source = (lane % group) * cycles + (target + cycle)
            for block in range(-(-groups // per_block)):
                value = jnp.zeros((pc, LANES), f32)
                for at in range(block * per_block, min(groups, (block + 1) * per_block)):
                    piece = jnp.take_along_axis(held[at], source, axis=1)
                    value = jnp.where(lane // group == at % per_block, piece, value)
                lanes = slice(block * LANES, (block + 1) * LANES)
                out_refs[shift][cycle, :, lanes] = value.astype(bf16)


def legendre_sums(legendre, coefficients, band_index, n_aa):
    waves_local, cycles, degrees = legendre.shape
    pc = coefficients.shape[2] * coefficients.shape[3]
    group = LANES // cycles
    per_step = 32 // group if waves_local % 32 == 0 else 16 // group
    rows = group * per_step
    steps = waves_local // rows
    blocks = -(-waves_local // LANES)
    wave_lanes = -(-waves_local * n_aa // LANES) * LANES
    shape = (n_aa, waves_local, cycles, pc, group, per_step, wave_lanes)
    return pl.pallas_call(
        functools.partial(legendre_kernel, shape),
        in_specs=[SMEM_SPEC] + [pl.BlockSpec(memory_space=pltpu.HBM)] * 2,
        out_specs=[vmem_spec()] * n_aa,
        out_shape=[jax.ShapeDtypeStruct((cycles // n_aa, pc, blocks * LANES), bf16)] * n_aa,
        scratch_shapes=[
            pltpu.VMEM((steps, rows * cycles, degrees), bf16),
            pltpu.VMEM((steps, rows * pc, degrees), bf16),
            pltpu.VMEM((waves_local // group, pc, LANES), f32),
            pltpu.SemaphoreType.DMA((2, steps)),
        ],
        compiler_params=params(0, 52),
        cost_estimate=cost(7_000_000_000, 20_000_000),
        name="legendre",
    )(
        band_index,
        legendre.reshape(steps, rows * cycles, degrees),
        coefficients.reshape(steps, rows * pc, degrees),
    )


def sine_cosine(wave, slot, points, inverse):
    product = wave * slot
    remain = product - jnp.floor(product * inverse + 0.5) * points
    turn = remain / points
    quarter = jnp.floor(4.0 * turn + 0.5)
    angle = (turn - 0.25 * quarter) * two_pi
    square = angle * angle
    sine = angle * (
        1.0
        + square
        * (-1.0 / 6.0 + square * (1.0 / 120.0 + square * (-1.0 / 5040.0 + square / 362880.0)))
    )
    cosine = 1.0 + square * (
        -0.5 + square * (1.0 / 24.0 + square * (-1.0 / 720.0 + square / 40320.0))
    )
    side = jnp.abs(quarter) == 1.0
    back = jnp.abs(quarter) == 2.0
    cosine_out = jnp.where(side, -quarter * sine, jnp.where(back, -cosine, cosine))
    sine_out = jnp.where(side, quarter * cosine, jnp.where(back, -sine, sine))
    return sine_out, cosine_out


def build_tables(shape, band, points, slot, coarse, write):
    n_aa, waves_local, fine_rows = shape
    coarse_local = waves_local // fine_rows
    coarse_rows, width = coarse.shape[1], slot.shape[1]
    points_row = jnp.full((1, width), points, f32)
    inverse = 1.0 / points_row
    active = slot < points_row
    fine = lax.broadcasted_iota(jnp.int32, (fine_rows, width), 0).astype(f32)
    sine_fine, cosine_fine = sine_cosine(fine, slot, points_row, inverse)
    row = lax.broadcasted_iota(jnp.int32, (coarse_rows, width), 0)
    wave = jnp.zeros((coarse_rows, width), jnp.int32)
    for shift in range(n_aa):
        first = lax.rem(band - shift + n_aa, n_aa) * waves_local
        inside = (row >= shift * coarse_local) & (row < (shift + 1) * coarse_local)
        wave = jnp.where(inside, first + (row - shift * coarse_local) * fine_rows, wave)
    sine_coarse, cosine_coarse = sine_cosine(wave.astype(f32), slot, points_row, inverse)
    coarse[0] = jnp.where(active, 2.0 * cosine_coarse, 0.0)
    coarse[1] = jnp.where(active, -2.0 * sine_coarse, 0.0)
    for shift in range(n_aa):
        first = lax.rem(band - shift + n_aa, n_aa) * waves_local
        for step in range(coarse_local):
            at = shift * coarse_local + step
            cosine_at = coarse[0, at : at + 1, :]
            sine_at = coarse[1, at : at + 1, :]
            cosine_part = cosine_at * cosine_fine + sine_at * sine_fine
            sine_part = sine_at * cosine_fine - cosine_at * sine_fine
            if step == 0:
                weight = jnp.where(fine + first.astype(f32) == 0.0, 0.5, 1.0)
                cosine_part = cosine_part * weight
                sine_part = sine_part * weight
            rows = slice(at * fine_rows, (at + 1) * fine_rows)
            write(rows, cosine_part.astype(bf16), sine_part.astype(bf16))
        yield shift


def table_shape(n_aa, waves_local):
    fine_rows = 32 if waves_local % 32 == 0 else 16
    coarse_rows = -(-(n_aa * waves_local // fine_rows) // 8) * 8
    return (n_aa, waves_local, fine_rows), coarse_rows


def wind_table_kernel(shape, sizes, where_ref, count_ref, column_ref, out_ref, coarse):
    n_in, cycles, cycle_rows, columns_local = sizes
    band, column = where_ref[0], where_ref[1]
    cycle = pl.program_id(0)
    points = count_ref[band * cycles + cycle].astype(f32)
    lane = lax.broadcasted_iota(jnp.int32, (1, LANES), 1)
    per_block = LANES // columns_local
    parts = []
    for inner in range(n_in):
        owner = jnp.bitwise_xor(column, inner)
        part = jnp.zeros((1, LANES), jnp.int32)
        for row in range(cycle_rows):
            source = column_ref[pl.ds(cycle * cycle_rows + row, 1), :]
            piece = source[:, :LANES]
            for block in range(1, source.shape[1] // LANES):
                piece = jnp.where(
                    owner // per_block == block,
                    source[:, block * LANES : (block + 1) * LANES],
                    piece,
                )
            turn = lax.rem(row - lax.rem(owner, per_block) + per_block, per_block)
            piece = pltpu.roll(piece, turn * columns_local, 1)
            part = jnp.where(lane // columns_local == row, piece, part)
        parts.append(part)
    slot = jnp.concatenate(parts, axis=1).astype(f32)

    def write(rows, cosine_part, sine_part):
        out_ref[0, 0, rows, :] = cosine_part
        out_ref[0, 1, rows, :] = sine_part

    for _ in build_tables(shape, band, points, slot, coarse, write):
        pass


def wind_tables(wind_column, counts, where, n_aa, waves_local, n_in, sizes):
    cycles = sizes[0]
    shape, coarse_rows = table_shape(n_aa, waves_local)
    waves, width = n_aa * waves_local, n_in * LANES
    return pl.pallas_call(
        functools.partial(wind_table_kernel, shape, (n_in,) + sizes),
        grid=(cycles,),
        in_specs=[SMEM_SPEC, SMEM_SPEC, vmem_spec()],
        out_specs=pl.BlockSpec((1, 2, waves, width), lambda i: (i, 0, 0, 0)),
        out_shape=jax.ShapeDtypeStruct((cycles, 2, waves, width), bf16),
        scratch_shapes=[pltpu.VMEM((2, coarse_rows, width), f32)],
        compiler_params=params(),
        cost_estimate=cost(1_700_000_000, 3_000_000),
        name="wind_tables",
    )(where, counts, wind_column)


def stack_rows(pieces):
    if pieces[0].shape[0] % 16 == 0:
        return jnp.concatenate(pieces, axis=0)
    return jnp.concatenate([piece.astype(f32) for piece in pieces], axis=0).astype(bf16)


def synthesis_kernel(shape, n_out, n_in, where_ref, count_ref, *refs):
    fourier, (out_ref, coarse, table) = refs[:n_in], refs[n_in:]
    _, waves_local, _ = shape
    band, column = where_ref[0], where_ref[1]
    cycle = pl.program_id(0)
    points = count_ref[band * pl.num_programs(0) + cycle].astype(f32)
    levels, width = out_ref.shape[2:]
    pc = fourier[0].shape[3]
    slot = column * width + lax.broadcasted_iota(jnp.int32, (1, width), 1)

    def write(rows, cosine_part, sine_part):
        table[0, rows, :] = cosine_part
        table[1, rows, :] = sine_part

    cosine_sum = None
    sine_sum = None
    for shift in build_tables(shape, band, points, slot.astype(f32), coarse, write):
        left = stack_rows(
            [
                fourier[inner][outer, shift, 0, :, :waves_local]
                for inner in range(n_in)
                for outer in range(n_out)
            ]
        )
        rows = slice(shift * waves_local, (shift + 1) * waves_local)
        cosine_part = jnp.dot(left, table[0, rows, :], preferred_element_type=f32)
        sine_part = jnp.dot(left, table[1, rows, :], preferred_element_type=f32)
        cosine_sum = cosine_part if cosine_sum is None else cosine_sum + cosine_part
        sine_sum = sine_part if sine_sum is None else sine_sum + sine_part
    for inner in range(n_in):
        for outer in range(n_out):
            at = (inner * n_out + outer) * pc
            value = cosine_sum[at : at + levels] + sine_sum[at + levels : at + pc]
            source = jnp.bitwise_xor(column, outer * n_in + inner)
            out_ref[0, source] = value.astype(bf16)


def synthesis(fourier, counts, where, n_aa, waves_local, n_in, width):
    n_out, _, cycles, pc, lanes = fourier[0].shape
    levels = pc // 2
    n_ba = n_out * n_in
    shape, coarse_rows = table_shape(n_aa, waves_local)
    block = pl.BlockSpec((n_out, n_aa, 1, pc, lanes), lambda i: (0, 0, i, 0, 0))
    return pl.pallas_call(
        functools.partial(synthesis_kernel, shape, n_out, n_in),
        grid=(cycles,),
        in_specs=[SMEM_SPEC, SMEM_SPEC] + [block] * n_in,
        out_specs=pl.BlockSpec((1, n_ba, levels, width), lambda i: (i, 0, 0, 0)),
        out_shape=jax.ShapeDtypeStruct((cycles, n_ba, levels, width), bf16),
        scratch_shapes=[
            pltpu.VMEM((2, coarse_rows, width), f32),
            pltpu.VMEM((2, n_aa * waves_local, width), bf16),
        ],
        compiler_params=params(),
        cost_estimate=cost(3_500_000_000, 2_000_000),
        name="synthesis",
    )(where, counts, *fourier)


def pick_kernel(shape, where_ref, fourier_ref, table_ref, *out_refs):
    n_aa, waves_local, n_in = shape
    outer_at = where_ref[1] // n_in
    cycles = out_refs[0].shape[0]
    pc = fourier_ref.shape[3]
    levels = pc // 2
    for cycle in range(cycles):
        total = None
        for shift in range(n_aa):
            left = fourier_ref[outer_at, shift, cycle][:, :waves_local]
            rows = slice(shift * waves_local, (shift + 1) * waves_local)
            cosine_part = jnp.dot(left, table_ref[cycle, 0, rows, :], preferred_element_type=f32)
            sine_part = jnp.dot(left, table_ref[cycle, 1, rows, :], preferred_element_type=f32)
            part = cosine_part[0:1] + sine_part[levels : levels + 1]
            total = part if total is None else total + part
        wind = wind_scale * total.astype(bf16).astype(f32)
        for inner, out_ref in enumerate(out_refs):
            out_ref[cycle : cycle + 1, :] = wind[:, inner * LANES : (inner + 1) * LANES]


def pick_winds(fourier, table, where, n_aa, waves_local, n_in):
    _, _, cycles, _, _ = fourier.shape
    return pl.pallas_call(
        functools.partial(pick_kernel, (n_aa, waves_local, n_in)),
        in_specs=[SMEM_SPEC] + [vmem_spec()] * 2,
        out_specs=[vmem_spec()] * n_in,
        out_shape=[jax.ShapeDtypeStruct((cycles, LANES), f32)] * n_in,
        compiler_params=params(0),
        cost_estimate=cost(1_000_000_000, 2_000_000),
        name="pick",
    )(where, fourier, table)


def bin_table(parts):
    bins = np.arange(NDIR * NFREQ)
    directions, freq_index = bins // NFREQ, bins % NFREQ
    heading = two_pi * (directions + 0.5) / NDIR
    period_ratio = np.exp(-math.log(1.1) * (35.0 / (NFREQ - 1)) * freq_index)
    frequency = base_freq / period_ratio
    drift_east = courant * period_ratio * np.cos(heading)
    drift_north = courant * period_ratio * np.sin(heading)
    inverse_speed = two_pi * frequency / gravity
    bin_width = 0.1 * frequency * (two_pi / NDIR)
    east_pos, east_neg = np.maximum(drift_east, 0.0), -np.minimum(drift_east, 0.0)
    north_pos, north_neg = np.maximum(drift_north, 0.0), -np.minimum(drift_north, 0.0)
    rows = [
        1.0 - east_pos - east_neg - north_pos - north_neg,
        east_pos,
        east_neg,
        north_pos,
        north_neg,
        np.cos(heading) * inverse_speed,
        np.sin(heading) * inverse_speed,
        bin_width,
        dissipation * (frequency / mid_freq),
    ]
    rows += [np.zeros_like(frequency)] * (16 - len(rows))
    table = np.stack(rows).astype(np.float32).reshape(16, parts, -1)
    return np.ascontiguousarray(table.transpose(1, 0, 2))


def column_of(values, at):
    lane = lax.broadcasted_iota(jnp.int32, values.shape, 1)
    return jnp.sum(jnp.where(lane == at, values, 0.0), axis=1, keepdims=True)


def transposed_mask(mask_ref, padded):
    rows, columns = mask_ref.shape
    padded[...] = jnp.zeros_like(padded)
    padded[:rows, :columns] = mask_ref[...].astype(f32)
    return jnp.transpose(padded[...])


def pack_kernel(n_aa, where_ref, spectra_ref, mask_ref, *refs):
    row_refs, (west_ref, east_ref, padded) = refs[:-3], refs[-3:]
    rows, columns, bins = spectra_ref.shape
    turned = transposed_mask(mask_ref, padded)
    starts = [0, rows - 2]
    if n_aa == 2:
        starts = [jnp.where(where_ref[0] == 0, rows - 2, 0)]
    for start, row_ref in zip(starts, row_refs):
        for at in range(2):
            own = column_of(turned, start + at)[:columns]
            row_ref[at, :, :bins] = spectra_ref[start + at] * own
            row_ref[at, :, bins:] = own
    mask = mask_ref[...].astype(f32)
    for side_ref, start in ((west_ref, 0), (east_ref, columns - 2)):
        for at in range(2):
            own = column_of(mask, start + at)
            side_ref[:, at, :bins] = spectra_ref[:, start + at, :] * own
            side_ref[:, at, bins:] = own


def pack(where, spectra, mask, n_aa):
    rows, columns, bins = spectra.shape
    n_rows = 1 if n_aa == 2 else 2
    return pl.pallas_call(
        functools.partial(pack_kernel, n_aa),
        in_specs=[SMEM_SPEC] + [vmem_spec()] * 2,
        out_specs=[vmem_spec()] * (n_rows + 2),
        out_shape=[jax.ShapeDtypeStruct((2, columns, bins + 1), f32)] * n_rows
        + [jax.ShapeDtypeStruct((rows, 2, bins + 1), f32)] * 2,
        scratch_shapes=[pltpu.VMEM((LANES, LANES), f32)],
        compiler_params=params(0),
        cost_estimate=cost(600_000_000, 500_000),
        name="pack",
    )(where, spectra, mask)


def rows_beyond(n_aa, where_ref, low_ref, high_ref, at):
    low = jnp.where(where_ref[0] > 0, low_ref[at], 0.0)
    high = jnp.where(where_ref[0] < n_aa - 1, high_ref[1 - at], 0.0)
    return low, high


def sides_kernel(n_aa, where_ref, low_ref, high_ref, west_ref, east_ref, out_west, out_east):
    rows, _, _ = west_ref.shape
    columns = low_ref.shape[1]
    low, high = rows_beyond(n_aa, where_ref, low_ref, high_ref, 1)
    for side_ref, out_ref, cut in (
        (west_ref, out_west, slice(0, 2)),
        (east_ref, out_east, slice(columns - 2, columns)),
    ):
        out_ref[0] = low[cut]
        out_ref[1 : rows + 1] = side_ref[...]
        out_ref[rows + 1] = high[cut]


def pack_sides(where, low, high, west, east, n_aa):
    rows, _, count = west.shape
    return pl.pallas_call(
        functools.partial(sides_kernel, n_aa),
        in_specs=[SMEM_SPEC] + [vmem_spec()] * 4,
        out_specs=[vmem_spec()] * 2,
        out_shape=[jax.ShapeDtypeStruct((rows + 2, 2, count), f32)] * 2,
        compiler_params=params(0),
        cost_estimate=cost(300_000_000, 500_000),
        name="pack_sides",
    )(where, low, high, west, east)


def advect_kernel(
    n_aa,
    where_ref,
    bins_ref,
    spectra_ref,
    mask_ref,
    low_ref,
    high_ref,
    west_ref,
    east_ref,
    out_ref,
    first,
    second,
    padded,
):
    rows, columns, bins = spectra_ref.shape
    half = where_ref[2]
    wide = columns + 2 * PAD
    turned = transposed_mask(mask_ref, padded)
    edge = jnp.zeros((PAD, bins), f32)
    for row in range(rows + 4):
        first[row, 0:PAD] = edge
        first[row, PAD + columns :] = edge
    inside = slice(PAD, PAD + columns)
    low_far, high_far = rows_beyond(n_aa, where_ref, low_ref, high_ref, 0)
    low_near, high_near = rows_beyond(n_aa, where_ref, low_ref, high_ref, 1)
    first[0, inside] = low_far[:, :bins]
    first[1, inside] = low_near[:, :bins]
    first[rows + 2, inside] = high_near[:, :bins]
    first[rows + 3, inside] = high_far[:, :bins]
    masks = [low_near[:, bins:]]
    for row in range(rows):
        masks.append(column_of(turned, row)[:columns])
        first[row + 2, inside] = spectra_ref[row] * masks[-1]
    masks.append(high_near[:, bins:])
    first[1 : rows + 3, PAD - 2 : PAD] = west_ref[:, :, :bins]
    first[1 : rows + 3, PAD + columns : PAD + columns + 2] = east_ref[:, :, :bins]
    keep, east_pos, east_neg, north_pos, north_neg = (
        bins_ref[half, at : at + 1] for at in range(5)
    )

    def update(source, at):
        centre = source[at]
        western = pltpu.roll(centre, 1, 0)
        eastern = pltpu.roll(centre, wide - 1, 0)
        return (
            keep * centre
            + east_pos * western
            + east_neg * eastern
            + north_pos * source[at - 1]
            + north_neg * source[at + 1]
        )

    for row in range(rows + 2):
        value = update(first, row + 1)
        second[row, 0:PAD] = value[0:PAD] * west_ref[row, 1:2, bins:]
        second[row, inside] = value[inside] * masks[row]
        second[row, PAD + columns :] = value[PAD + columns :] * east_ref[row, 0:1, bins:]
    for row in range(rows):
        value = update(second, row + 1)
        out_ref[row] = value[inside] * masks[row + 1]


def advect(where, bins, spectra, mask, low, high, west, east, n_aa):
    rows, columns, count = spectra.shape
    wide = columns + 2 * PAD
    return pl.pallas_call(
        functools.partial(advect_kernel, n_aa),
        in_specs=[SMEM_SPEC] + [vmem_spec()] * 7,
        out_specs=vmem_spec(),
        out_shape=jax.ShapeDtypeStruct(spectra.shape, f32),
        scratch_shapes=[
            pltpu.VMEM((rows + 4, wide, count), f32),
            pltpu.VMEM((rows + 2, wide, count), f32),
            pltpu.VMEM((LANES, LANES), f32),
        ],
        compiler_params=params(0),
        cost_estimate=cost(2_600_000_000, 4_000_000),
        name="advect",
    )(where, bins, spectra, mask, low, high, west, east)


def across(sent, axis):
    count = lax.axis_size(axis)
    if len(sent) == 1:
        got = lax.ppermute(sent[0], axis, [(0, 1), (1, 0)])
        return got, got
    forward = [(i, i + 1) for i in range(count - 1)]
    backward = [(target, source) for source, target in forward]
    return lax.ppermute(sent[1], axis, forward), lax.ppermute(sent[0], axis, backward)


def as_columns(rows_by_lanes):
    rows = rows_by_lanes.shape[0]
    if rows % 8:
        rows_by_lanes = jnp.concatenate(
            [rows_by_lanes, jnp.zeros((8 - rows % 8, LANES), f32)], axis=0
        )
    return jnp.transpose(rows_by_lanes)


def stress_kernel(
    n_in, where_ref, bins_ref, density_ref, own_ref, own_far_ref, other_ref, other_far_ref,
    sums_ref, points_ref
):
    cycles = own_ref.shape[0]
    rows, _, bins = density_ref.shape
    cycle_rows = rows // cycles
    half = where_ref[2]
    holds = lax.rem(where_ref[1], n_in) == 0
    own = jnp.where(holds, own_ref[...], own_far_ref[...])
    other = jnp.where(holds, other_ref[...], other_far_ref[...])
    east_rows = jnp.where(half == 0, own, other)
    north_rows = jnp.where(half == 0, other, own)
    points_ref[0] = east_rows
    points_ref[1] = north_rows
    points_ref[2] = drag_coef * (own * own + other * other) + stress_floor
    east, north = as_columns(east_rows), as_columns(north_rows)
    along_cos, along_sin, width = (bins_ref[half, at : at + 1] for at in (5, 6, 7))
    lane = lax.broadcasted_iota(jnp.int32, (LANES, LANES), 1)
    sums = jnp.zeros((LANES, LANES), f32)
    for cycle in range(cycles):
        density = density_ref[cycle * cycle_rows : (cycle + 1) * cycle_rows].reshape(LANES, bins)
        alignment = (
            east[:, cycle : cycle + 1] * along_cos + north[:, cycle : cycle + 1] * along_sin
        )
        weighted = density * width
        gain = growth * jnp.maximum(alignment - 1.0, 0.0)
        energy = jnp.sum(weighted, axis=1, keepdims=True)
        stress = jnp.sum(gain * alignment * weighted, axis=1, keepdims=True)
        sums = jnp.where(lane == cycle, stress, sums)
        sums = jnp.where(lane == cycles + cycle, energy, sums)
    turned = jnp.transpose(sums)
    sums_ref[0] = turned[:cycles]
    sums_ref[1] = turned[cycles : 2 * cycles]


def stress_sums(where, bins, density, winds, n_in):
    cycles = winds[0].shape[0]
    return pl.pallas_call(
        functools.partial(stress_kernel, n_in),
        in_specs=[SMEM_SPEC] + [vmem_spec()] * 6,
        out_specs=[vmem_spec()] * 2,
        out_shape=[
            jax.ShapeDtypeStruct((2, cycles, LANES), f32),
            jax.ShapeDtypeStruct((3, cycles, LANES), f32),
        ],
        compiler_params=params(0),
        cost_estimate=cost(1_500_000_000, 2_000_000),
        name="stress",
    )(where, bins, density, *winds)


def spectra_kernel(where_ref, bins_ref, density_ref, points_ref, sums_ref, far_ref, out_ref):
    cycle = pl.program_id(0)
    half = where_ref[2]
    cycle_rows, columns, bins = density_ref.shape
    scaled = (sums_ref[1] + far_ref[1]) * (1.0 / energy_ref)
    row = lax.broadcasted_iota(jnp.int32, (8, LANES), 0)

    def own_row(values):
        mine = lax.broadcasted_iota(jnp.int32, values.shape, 0) == cycle
        return jnp.sum(jnp.where(mine, values, 0.0), axis=0, keepdims=True)

    picked = jnp.where(
        row == 0,
        own_row(points_ref[0]),
        jnp.where(row == 1, own_row(points_ref[1]), own_row(scaled * scaled)),
    )
    picked = jnp.transpose(picked)
    along_cos, along_sin, decay = (bins_ref[half, at : at + 1] for at in (5, 6, 8))
    density = density_ref[...].reshape(LANES, bins)
    alignment = picked[:, 0:1] * along_cos + picked[:, 1:2] * along_sin
    gain = growth * jnp.maximum(alignment - 1.0, 0.0)
    value = density * (1.0 + gain) / (1.0 + decay * picked[:, 2:3])
    out_ref[...] = value.reshape(cycle_rows, columns, bins)


def final_spectra(where, bins, density, points, sums, far):
    cycles = points.shape[1]
    rows, columns, count = density.shape
    block = pl.BlockSpec((rows // cycles, columns, count), lambda i: (i, 0, 0))
    return pl.pallas_call(
        spectra_kernel,
        grid=(cycles,),
        in_specs=[SMEM_SPEC, vmem_spec(), block] + [vmem_spec()] * 3,
        out_specs=block,
        out_shape=jax.ShapeDtypeStruct(density.shape, f32),
        compiler_params=params(1),
        cost_estimate=cost(2_500_000_000, 3_000_000),
        name="spectra",
    )(where, bins, density, points, sums, far)


def charnock_kernel(shape, where_ref, count_ref, source_ref, *refs):
    columns_local, total_columns, order = shape
    rough_refs, out_ref = refs[:-1], refs[-1]
    column = where_ref[1]
    cycles, width = source_ref.shape
    cycle_rows = LANES // columns_local
    base = column * width
    row = lax.broadcasted_iota(jnp.int32, (cycles, LANES), 0)
    points = jnp.zeros((cycles, LANES), jnp.int32)
    for cycle in range(cycles):
        points = jnp.where(row == cycle, count_ref[where_ref[0] * cycles + cycle], points)
    lane = lax.broadcasted_iota(jnp.int32, (cycles, LANES), 1)
    for part in range(width // LANES):
        at = slice(part * LANES, (part + 1) * LANES)
        source = source_ref[:, at]
        band_row = source // total_columns
        source_column = source - band_row * total_columns
        owner = source_column // columns_local
        within = (band_row - row * cycle_rows) * columns_local + (
            source_column - owner * columns_local
        )
        within = jnp.clip(within, 0, LANES - 1)
        value = jnp.zeros((cycles, LANES), f32)
        for rough_ref, distances in zip(rough_refs, order):
            for at_piece, distance in enumerate(distances):
                found = jnp.take_along_axis(rough_ref[at_piece], within, axis=1)
                value = jnp.where(owner == jnp.bitwise_xor(column, distance), found, value)
        out_ref[:, at] = jnp.where(lane + (base + part * LANES) < points, value, 0.0)


def charnock_of(where, counts, pieces, order, source, columns_local):
    total_columns = columns_local * sum(len(distances) for distances in order)
    return pl.pallas_call(
        functools.partial(charnock_kernel, (columns_local, total_columns, order)),
        in_specs=[SMEM_SPEC, SMEM_SPEC] + [vmem_spec()] * (1 + len(pieces)),
        out_specs=vmem_spec(),
        out_shape=jax.ShapeDtypeStruct(source.shape, f32),
        compiler_params=params(0),
        cost_estimate=cost(1_000_000_000, 100_000),
        name="charnock",
    )(where, counts, source, *pieces)


def exchange(value, axis, distance):
    count = lax.axis_size(axis)
    return lax.ppermute(value, axis, [(i, i ^ distance) for i in range(count)])


def exchange_both(value, n_comp, n_ba):
    pairs = [
        (half * n_ba + i, (half ^ 1) * n_ba + (i ^ 1))
        for half in range(n_comp)
        for i in range(n_ba)
    ]
    return lax.ppermute(value, ("comp", "ba"), pairs)


def per_device(
    legendre, coefficients, cycle_points, spectra, sea_mask, wind_column, roughness_source
):
    n_aa, n_ba = lax.axis_size("aa"), lax.axis_size("ba")
    n_comp = lax.axis_size("comp")
    band_index = lax.axis_index("aa")
    column_index = lax.axis_index("ba")
    half_index = lax.axis_index("comp")
    where = jnp.stack([band_index, column_index, half_index]).astype(jnp.int32)
    waves_local, cycles_all, _ = legendre.shape
    cycles = cycles_all // n_aa
    rows_local, columns_local, _ = spectra.shape
    cycle_rows = rows_local // cycles
    n_in = 2
    n_out = n_ba // n_in
    slots_local = LON // n_ba
    counts = cycle_points
    bins = jnp.asarray(bin_table(n_comp))

    fourier = legendre_sums(legendre, coefficients, where, n_aa)

    *row_sides, west, east = pack(where, spectra, sea_mask, n_aa)
    low, high = across(row_sides, "aa")
    west, east = pack_sides(where, low, high, west, east, n_aa)
    west, east = across([west, east], "ba")
    density = advect(where, bins, spectra, sea_mask, low, high, west, east, n_aa)
    wind_table = wind_tables(
        wind_column, counts, where, n_aa, waves_local, n_in,
        (cycles, cycle_rows, columns_local),
    )

    parts = [fourier[0]]
    for shift in range(1, n_aa):
        pairs = [(i, (i + shift) % n_aa) for i in range(n_aa)]
        parts.append(lax.ppermute(fourier[shift], "aa", pairs))
    parts = jnp.stack(parts)
    outer = [parts]
    for k in range(1, n_out):
        outer.append(exchange(parts, "ba", n_in * k))
    outer = jnp.stack(outer)

    picked = pick_winds(outer, wind_table, where, n_aa, waves_local, n_in)
    own_sent = exchange(picked[1], "ba", 1)
    other_sent = exchange_both(picked[1], n_comp, n_ba)
    other_here = exchange(picked[0], "comp", 1)
    inner = [outer]
    for k in range(1, n_in):
        inner.append(exchange(outer, "ba", k))

    winds = (picked[0], own_sent, other_here, other_sent)
    sums, points = stress_sums(where, bins, density, winds, n_in)
    far = exchange(sums, "comp", 1)
    roughness = jnp.sqrt(1.0 + stress_coef * (sums[0] + far[0]) / points[2])
    pieces, order = [roughness[None]], [(0,)]
    for distance in [n_in << k for k in range(n_out.bit_length() - 1)] + [1]:
        sent = jnp.concatenate(pieces, axis=0)
        pieces.append(exchange(sent, "ba", distance))
        order.append(tuple(far_at ^ distance for near in order for far_at in near))
    wave_spectra = final_spectra(where, bins, density, points, sums, far)
    grid_winds = synthesis(inner, counts, where, n_aa, waves_local, n_in, slots_local)
    grid_winds = grid_winds.reshape(1, cycles, -1, slots_local)
    charnock = charnock_of(
        where, counts, pieces, tuple(order), roughness_source, columns_local
    )
    return (grid_winds, wave_spectra, charnock)


def solution(mesh):
    in_specs = (
        P("aa", None, None),
        P("comp", "aa", None, "ba", None),
        P(),
        P("aa", "ba", "comp"),
        P("aa", "ba"),
        P("aa", None),
        P("aa", "ba"),
    )
    out_specs = (P("comp", "aa", None, "ba"), P("aa", "ba", "comp"), P("aa", "ba"))
    return jax.shard_map(
        per_device, mesh=mesh, in_specs=in_specs, out_specs=out_specs, check_vma=False
    )
```

```python
import functools
import math

import jax
import jax.numpy as jnp
import numpy as np
from jax import lax
from jax.experimental import pallas as pl
from jax.experimental.pallas import tpu as pltpu
from jax.sharding import PartitionSpec as P


LON = 4096
NDIR = 36
NFREQ = 36
LANES = 128

two_pi = 2.0 * math.pi
gravity = 9.81
base_freq = 0.04177
courant = 0.45
wind_scale = 10.0
growth = 0.05
dissipation = 0.5
energy_ref = 8.0
mid_freq = 0.2
stress_coef = 0.03
drag_coef = 0.0012
stress_floor = 0.02


bf16 = jnp.bfloat16
f32 = jnp.float32
SMEM_SPEC = pl.BlockSpec(memory_space=pltpu.SMEM)


def vmem_spec():
    return pl.BlockSpec(memory_space=pltpu.VMEM)


def params(grid_dims=1, mebibytes=16):
    return pltpu.CompilerParams(
        dimension_semantics=("arbitrary",) * grid_dims, vmem_limit_bytes=mebibytes * 1024 * 1024
    )


def cost(flops, nbytes):
    return pl.CostEstimate(flops=flops, bytes_accessed=nbytes, transcendentals=0)


def legendre_kernel(shape, where_ref, leg_hbm, coef_hbm, *refs):
    n_aa, waves_local, cycles, pc, group, per_step, wave_lanes = shape
    out_refs, (leg_all, coef_all, held, arrived) = refs[:n_aa], refs[n_aa:]
    steps = leg_all.shape[0]
    band = where_ref[0]
    band_cycles = cycles // n_aa
    per_block = LANES // group
    groups = waves_local // group

    def copies(step):
        return (
            pltpu.make_async_copy(leg_hbm.at[step], leg_all.at[step], arrived.at[0, step]),
            pltpu.make_async_copy(coef_hbm.at[step], coef_all.at[step], arrived.at[1, step]),
        )

    for step in range(steps):
        for copy in copies(step):
            copy.start()

    lane = lax.broadcasted_iota(jnp.int32, (pc, LANES), 1)
    row_wave = lax.broadcasted_iota(jnp.int32, (group * cycles, wave_lanes), 0) // cycles
    degree = lax.broadcasted_iota(jnp.int32, (group * cycles, wave_lanes), 1)
    ahead = degree - row_wave
    contract = (((1,), (1,)), ((), ()))

    def one_step(step, carry):
        for copy in copies(step):
            copy.wait()
        for part in range(per_step):
            index = step * per_step + part
            leg_rows = pl.ds(part * group * cycles, group * cycles)
            coef_rows = pl.ds(part * group * pc, group * pc)
            first = band * waves_local + index * group
            low = leg_all[step, leg_rows, :wave_lanes].astype(f32)
            low = jnp.where(ahead >= first, low, 0.0).astype(bf16)
            full = lax.dot_general(
                coef_all[step, coef_rows, :wave_lanes],
                low,
                contract,
                preferred_element_type=f32,
            ) + lax.dot_general(
                coef_all[step, coef_rows, wave_lanes:],
                leg_all[step, leg_rows, wave_lanes:],
                contract,
                preferred_element_type=f32,
            )
            own = full[:pc]
            for wave in range(1, group):
                own = jnp.where(lane // cycles == wave, full[wave * pc : (wave + 1) * pc], own)
            held[index] = own
        return carry

    lax.fori_loop(0, steps, one_step, 0)

    for shift in range(n_aa):
        target = lax.rem(band + shift, n_aa) * band_cycles
        for cycle in range(band_cycles):
            source = (lane % group) * cycles + (target + cycle)
            for block in range(-(-groups // per_block)):
                value = jnp.zeros((pc, LANES), f32)
                for at in range(block * per_block, min(groups, (block + 1) * per_block)):
                    piece = jnp.take_along_axis(held[at], source, axis=1)
                    value = jnp.where(lane // group == at % per_block, piece, value)
                lanes = slice(block * LANES, (block + 1) * LANES)
                out_refs[shift][cycle, :, lanes] = value.astype(bf16)


def legendre_sums(legendre, coefficients, band_index, n_aa):
    waves_local, cycles, degrees = legendre.shape
    pc = coefficients.shape[2] * coefficients.shape[3]
    group = LANES // cycles
    per_step = 32 // group if waves_local % 32 == 0 else 16 // group
    rows = group * per_step
    steps = waves_local // rows
    blocks = -(-waves_local // LANES)
    wave_lanes = -(-waves_local * n_aa // LANES) * LANES
    shape = (n_aa, waves_local, cycles, pc, group, per_step, wave_lanes)
    return pl.pallas_call(
        functools.partial(legendre_kernel, shape),
        in_specs=[SMEM_SPEC] + [pl.BlockSpec(memory_space=pltpu.HBM)] * 2,
        out_specs=[vmem_spec()] * n_aa,
        out_shape=[jax.ShapeDtypeStruct((cycles // n_aa, pc, blocks * LANES), bf16)] * n_aa,
        scratch_shapes=[
            pltpu.VMEM((steps, rows * cycles, degrees), bf16),
            pltpu.VMEM((steps, rows * pc, degrees), bf16),
            pltpu.VMEM((waves_local // group, pc, LANES), f32),
            pltpu.SemaphoreType.DMA((2, steps)),
        ],
        compiler_params=params(0, 52),
        cost_estimate=cost(7_000_000_000, 20_000_000),
        name="legendre",
    )(
        band_index,
        legendre.reshape(steps, rows * cycles, degrees),
        coefficients.reshape(steps, rows * pc, degrees),
    )


def sine_cosine(wave, slot, points, inverse):
    product = wave * slot
    remain = product - jnp.floor(product * inverse + 0.5) * points
    turn = remain * inverse
    quarter = jnp.floor(4.0 * turn + 0.5)
    angle = (turn - 0.25 * quarter) * two_pi
    square = angle * angle
    sine = angle * (
        1.0
        + square
        * (-1.0 / 6.0 + square * (1.0 / 120.0 + square * (-1.0 / 5040.0 + square * (1.0 / 362880.0))))
    )
    cosine = 1.0 + square * (
        -0.5 + square * (1.0 / 24.0 + square * (-1.0 / 720.0 + square * (1.0 / 40320.0)))
    )
    side = jnp.abs(quarter) == 1.0
    back = jnp.abs(quarter) == 2.0
    cosine_out = jnp.where(side, -quarter * sine, jnp.where(back, -cosine, cosine))
    sine_out = jnp.where(side, quarter * cosine, jnp.where(back, -sine, sine))
    return sine_out, cosine_out


def build_tables(shape, band, points, slot, scratch, write):
    n_aa, waves_local, fine_rows = shape
    coarse, fine = scratch
    coarse_local = waves_local // fine_rows
    coarse_rows, width = coarse.shape[1], slot.shape[1]
    points_row = jnp.full((1, width), points, f32)
    inverse = 1.0 / points_row
    active = slot < points_row
    few = lax.broadcasted_iota(jnp.int32, (8, width), 0).astype(f32)
    sine_few, cosine_few = sine_cosine(few, slot, points_row, inverse)
    firsts = [lax.rem(band - shift + n_aa, n_aa) * waves_local for shift in range(n_aa)]
    eights = fine_rows // 8
    row = lax.broadcasted_iota(jnp.int32, (coarse_rows, width), 0)
    wave = (row + 1) * 8
    for shift in range(n_aa):
        wave = jnp.where(row == eights + shift, firsts[shift], wave)
    sine_coarse, cosine_coarse = sine_cosine(wave.astype(f32), slot, points_row, inverse)
    scale = jnp.where(row < eights, 1.0, jnp.where(active, 2.0, 0.0))
    coarse[0] = scale * cosine_coarse
    coarse[1] = scale * sine_coarse
    for eight in range(eights):
        rows = slice(eight * 8, (eight + 1) * 8)
        if eight == 0:
            fine[0, rows], fine[1, rows] = cosine_few, sine_few
            continue
        cosine_at = coarse[0, eight - 1 : eight, :]
        sine_at = coarse[1, eight - 1 : eight, :]
        fine[0, rows] = cosine_few * cosine_at - sine_few * sine_at
        fine[1, rows] = sine_few * cosine_at + cosine_few * sine_at
    index = lax.broadcasted_iota(jnp.int32, (fine_rows, LANES), 0)
    for shift in range(n_aa):
        at = eights + shift
        weight = jnp.where(index + firsts[shift] == 0, 0.5, 1.0)
        for start in range(0, width, LANES):
            lanes = slice(start, start + LANES)
            cosine_step = coarse[0, eights - 1 : eights, lanes]
            sine_step = coarse[1, eights - 1 : eights, lanes]
            twice = jnp.broadcast_to(2.0 * cosine_step, (fine_rows, LANES))
            cosine_at, sine_at = coarse[0, at : at + 1, lanes], coarse[1, at : at + 1, lanes]
            cosine_fine, sine_fine = fine[0, :, lanes], fine[1, :, lanes]
            cosine_now = cosine_at * cosine_fine - sine_at * sine_fine
            sine_now = -(sine_at * cosine_fine + cosine_at * sine_fine)
            cosine_old = sine_old = None
            for step in range(coarse_local):
                first_row = (shift * coarse_local + step) * fine_rows
                rows = slice(first_row, first_row + fine_rows)
                if step == 0:
                    write(rows, lanes, cosine_now * weight, sine_now * weight)
                    cosine_next = cosine_now * cosine_step + sine_now * sine_step
                    sine_next = sine_now * cosine_step - cosine_now * sine_step
                else:
                    write(rows, lanes, cosine_now, sine_now)
                    cosine_next = twice * cosine_now - cosine_old
                    sine_next = twice * sine_now - sine_old
                cosine_old, sine_old = cosine_now, sine_now
                cosine_now, sine_now = cosine_next, sine_next
        yield shift


def table_shape(n_aa, waves_local, width):
    fine_rows = 32 if waves_local % 32 == 0 else 16
    coarse_rows = -(-(fine_rows // 8 + n_aa) // 8) * 8
    scratch = [
        pltpu.VMEM((2, 2, coarse_rows, width), f32),
        pltpu.VMEM((2, 2, fine_rows, width), f32),
    ]
    return (n_aa, waves_local, fine_rows), scratch


def wind_table_kernel(shape, sizes, where_ref, count_ref, column_ref, out_ref, *scratch):
    n_in, cycles, cycle_rows, columns_local = sizes
    band, column = where_ref[0], where_ref[1]
    lane = lax.broadcasted_iota(jnp.int32, (1, LANES), 1)
    per_block = LANES // columns_local
    for cycle in range(cycles):
        points = count_ref[band * cycles + cycle].astype(f32)
        parts = []
        for inner in range(n_in):
            owner = jnp.bitwise_xor(column, inner)
            part = jnp.zeros((1, LANES), jnp.int32)
            for row in range(cycle_rows):
                at = cycle * cycle_rows + row
                source = column_ref[at : at + 1, :]
                piece = source[:, :LANES]
                for block in range(1, source.shape[1] // LANES):
                    piece = jnp.where(
                        owner // per_block == block,
                        source[:, block * LANES : (block + 1) * LANES],
                        piece,
                    )
                turn = lax.rem(row - lax.rem(owner, per_block) + per_block, per_block)
                piece = pltpu.roll(piece, turn * columns_local, 1)
                part = jnp.where(lane // columns_local == row, piece, part)
            parts.append(part)
        slot = jnp.concatenate(parts, axis=1).astype(f32)

        def write(rows, lanes, cosine_part, sine_part):
            out_ref[cycle, 0, rows, lanes] = cosine_part.astype(bf16)
            out_ref[cycle, 1, rows, lanes] = sine_part.astype(bf16)

        own = [ref.at[cycle % 2] for ref in scratch]
        for _ in build_tables(shape, band, points, slot, own, write):
            pass


def wind_tables(wind_column, counts, where, n_aa, waves_local, n_in, sizes):
    cycles = sizes[0]
    waves, width = n_aa * waves_local, n_in * LANES
    shape, scratch = table_shape(n_aa, waves_local, width)
    return pl.pallas_call(
        functools.partial(wind_table_kernel, shape, (n_in,) + sizes),
        in_specs=[SMEM_SPEC, SMEM_SPEC, vmem_spec()],
        out_specs=vmem_spec(),
        out_shape=jax.ShapeDtypeStruct((cycles, 2, waves, width), bf16),
        scratch_shapes=scratch,
        compiler_params=params(0),
        cost_estimate=cost(1_700_000_000, 3_000_000),
        name="wind_tables",
    )(where, counts, wind_column)


def grid_table_kernel(shape, cycles, where_ref, count_ref, out_ref, *scratch):
    band, column = where_ref[0], where_ref[1]
    width = out_ref.shape[3]
    slot = column * width + lax.broadcasted_iota(jnp.int32, (1, width), 1)
    for cycle in range(cycles):
        points = count_ref[band * cycles + cycle].astype(f32)

        def write(rows, lanes, cosine_part, sine_part):
            out_ref[cycle, 0, rows, lanes] = cosine_part.astype(bf16)
            out_ref[cycle, 1, rows, lanes] = sine_part.astype(bf16)

        own = [ref.at[cycle % 2] for ref in scratch]
        for _ in build_tables(shape, band, points, slot.astype(f32), own, write):
            pass


def grid_tables(counts, where, cycles, n_aa, waves_local, width):
    waves = n_aa * waves_local
    shape, scratch = table_shape(n_aa, waves_local, width)
    return pl.pallas_call(
        functools.partial(grid_table_kernel, shape, cycles),
        in_specs=[SMEM_SPEC, SMEM_SPEC],
        out_specs=vmem_spec(),
        out_shape=jax.ShapeDtypeStruct((cycles, 2, waves, width), bf16),
        scratch_shapes=scratch,
        compiler_params=params(0),
        cost_estimate=cost(2_000_000_000, 5_000_000),
        name="grid_tables",
    )(where, counts)


def stack_rows(pieces):
    if pieces[0].shape[0] % 16 == 0:
        return jnp.concatenate(pieces, axis=0)
    return jnp.concatenate([piece.astype(f32) for piece in pieces], axis=0).astype(bf16)


def synthesis_kernel(shape, n_out, n_in, where_ref, *refs):
    fourier, (table_ref, out_hbm, grid, done) = refs[:n_in], refs[n_in:]
    n_aa, waves_local = shape
    column = where_ref[1]
    cycles, _, levels, _ = grid.shape
    pc = fourier[0].shape[3]
    copies = []
    for cycle in range(cycles):
        cosine_sum = None
        sine_sum = None
        for shift in range(n_aa):
            left = stack_rows(
                [
                    fourier[inner][outer, shift, cycle, :, :waves_local]
                    for inner in range(n_in)
                    for outer in range(n_out)
                ]
            )
            rows = slice(shift * waves_local, (shift + 1) * waves_local)
            cosine_part = jnp.dot(left, table_ref[cycle, 0, rows, :], preferred_element_type=f32)
            sine_part = jnp.dot(left, table_ref[cycle, 1, rows, :], preferred_element_type=f32)
            cosine_sum = cosine_part if cosine_sum is None else cosine_sum + cosine_part
            sine_sum = sine_part if sine_sum is None else sine_sum + sine_part
        for inner in range(n_in):
            for outer in range(n_out):
                at = (inner * n_out + outer) * pc
                value = cosine_sum[at : at + levels] + sine_sum[at + levels : at + pc]
                source = jnp.bitwise_xor(column, outer * n_in + inner)
                grid[cycle, source] = value.astype(bf16)
        copies.append(
            pltpu.make_async_copy(grid.at[cycle], out_hbm.at[cycle], done.at[cycle])
        )
        copies[-1].start()
    for copy in copies:
        copy.wait()


def synthesis(fourier, table, where, n_aa, waves_local, n_in):
    n_out, _, cycles, pc, _ = fourier[0].shape
    levels = pc // 2
    width = table.shape[3]
    n_ba = n_out * n_in
    return pl.pallas_call(
        functools.partial(synthesis_kernel, (n_aa, waves_local), n_out, n_in),
        in_specs=[SMEM_SPEC] + [vmem_spec()] * (n_in + 1),
        out_specs=pl.BlockSpec(memory_space=pltpu.HBM),
        out_shape=jax.ShapeDtypeStruct((cycles, n_ba, levels, width), bf16),
        scratch_shapes=[
            pltpu.VMEM((cycles, n_ba, levels, width), bf16),
            pltpu.SemaphoreType.DMA((cycles,)),
        ],
        compiler_params=params(0),
        cost_estimate=cost(3_000_000_000, 2_000_000),
        name="synthesis",
    )(where, *fourier, table)


def pick_kernel(shape, where_ref, fourier_ref, table_ref, *out_refs):
    n_aa, waves_local, n_in = shape
    outer_at = where_ref[1] // n_in
    cycles = out_refs[0].shape[0]
    pc = fourier_ref.shape[3]
    levels = pc // 2
    for cycle in range(cycles):
        total = None
        for shift in range(n_aa):
            left = fourier_ref[outer_at, shift, cycle][:, :waves_local]
            rows = slice(shift * waves_local, (shift + 1) * waves_local)
            cosine_part = jnp.dot(left, table_ref[cycle, 0, rows, :], preferred_element_type=f32)
            sine_part = jnp.dot(left, table_ref[cycle, 1, rows, :], preferred_element_type=f32)
            part = cosine_part[0:1] + sine_part[levels : levels + 1]
            total = part if total is None else total + part
        wind = wind_scale * total.astype(bf16).astype(f32)
        for inner, out_ref in enumerate(out_refs):
            out_ref[cycle : cycle + 1, :] = wind[:, inner * LANES : (inner + 1) * LANES]


def pick_winds(fourier, table, where, n_aa, waves_local, n_in):
    _, _, cycles, _, _ = fourier.shape
    return pl.pallas_call(
        functools.partial(pick_kernel, (n_aa, waves_local, n_in)),
        in_specs=[SMEM_SPEC] + [vmem_spec()] * 2,
        out_specs=[vmem_spec()] * n_in,
        out_shape=[jax.ShapeDtypeStruct((cycles, LANES), f32)] * n_in,
        compiler_params=params(0),
        cost_estimate=cost(1_000_000_000, 2_000_000),
        name="pick",
    )(where, fourier, table)


def bin_table(parts):
    bins = np.arange(NDIR * NFREQ)
    directions, freq_index = bins // NFREQ, bins % NFREQ
    heading = two_pi * (directions + 0.5) / NDIR
    period_ratio = np.exp(-math.log(1.1) * (35.0 / (NFREQ - 1)) * freq_index)
    frequency = base_freq / period_ratio
    drift_east = courant * period_ratio * np.cos(heading)
    drift_north = courant * period_ratio * np.sin(heading)
    inverse_speed = two_pi * frequency / gravity
    bin_width = 0.1 * frequency * (two_pi / NDIR)
    east_pos, east_neg = np.maximum(drift_east, 0.0), -np.minimum(drift_east, 0.0)
    north_pos, north_neg = np.maximum(drift_north, 0.0), -np.minimum(drift_north, 0.0)
    rows = [
        1.0 - east_pos - east_neg - north_pos - north_neg,
        east_pos,
        east_neg,
        north_pos,
        north_neg,
        np.cos(heading) * inverse_speed,
        np.sin(heading) * inverse_speed,
        bin_width,
        dissipation * (frequency / mid_freq),
    ]
    rows += [np.zeros_like(frequency)] * (16 - len(rows))
    table = np.stack(rows).astype(np.float32).reshape(16, parts, -1)
    return np.ascontiguousarray(table.transpose(1, 0, 2))


def column_of(values, at):
    lane = lax.broadcasted_iota(jnp.int32, values.shape, 1)
    return jnp.sum(jnp.where(lane == at, values, 0.0), axis=1, keepdims=True)


def transposed_mask(mask_ref, padded):
    rows, columns = mask_ref.shape
    padded[...] = jnp.zeros_like(padded)
    padded[:rows, :columns] = mask_ref[...].astype(f32)
    return jnp.transpose(padded[...])


def pack_kernel(n_aa, where_ref, spectra_ref, mask_ref, *refs):
    row_refs, (west_ref, east_ref, padded) = refs[:-3], refs[-3:]
    rows, columns, bins = spectra_ref.shape
    turned = transposed_mask(mask_ref, padded)
    starts = [0, rows - 2]
    if n_aa == 2:
        starts = [jnp.where(where_ref[0] == 0, rows - 2, 0)]
    for start, row_ref in zip(starts, row_refs):
        for at in range(2):
            own = column_of(turned, start + at)[:columns]
            row_ref[at, :, :bins] = spectra_ref[start + at] * own
            row_ref[at, :, bins:] = own
    mask = mask_ref[...].astype(f32)
    for side_ref, start in ((west_ref, 0), (east_ref, columns - 2)):
        for at in range(2):
            own = column_of(mask, start + at)
            side_ref[at, :, :bins] = spectra_ref[:, start + at, :] * own
            side_ref[at, :, bins:] = own


def pack(where, spectra, mask, n_aa):
    rows, columns, bins = spectra.shape
    n_rows = 1 if n_aa == 2 else 2
    return pl.pallas_call(
        functools.partial(pack_kernel, n_aa),
        in_specs=[SMEM_SPEC] + [vmem_spec()] * 2,
        out_specs=[vmem_spec()] * (n_rows + 2),
        out_shape=[jax.ShapeDtypeStruct((2, columns, bins + 1), f32)] * n_rows
        + [jax.ShapeDtypeStruct((2, rows, bins + 1), f32)] * 2,
        scratch_shapes=[pltpu.VMEM((LANES, LANES), f32)],
        compiler_params=params(0),
        cost_estimate=cost(600_000_000, 500_000),
        name="pack",
    )(where, spectra, mask)


def rows_beyond(n_aa, where_ref, low_ref, high_ref, at):
    low = jnp.where(where_ref[0] > 0, low_ref[at], 0.0)
    high = jnp.where(where_ref[0] < n_aa - 1, high_ref[1 - at], 0.0)
    return low, high


def sides_kernel(n_aa, where_ref, low_ref, high_ref, west_ref, east_ref, out_west, out_east):
    rows = west_ref.shape[1]
    columns = low_ref.shape[1]
    low, high = rows_beyond(n_aa, where_ref, low_ref, high_ref, 1)
    for side_ref, out_ref, start in (
        (west_ref, out_west, 0),
        (east_ref, out_east, columns - 2),
    ):
        for at in range(2):
            cut = slice(start + at, start + at + 1)
            out_ref[at, 0:1] = low[cut]
            out_ref[at, 1 : rows + 1] = side_ref[at]
            out_ref[at, rows + 1 :] = high[cut]


def pack_sides(where, low, high, west, east, n_aa):
    _, rows, count = west.shape
    return pl.pallas_call(
        functools.partial(sides_kernel, n_aa),
        in_specs=[SMEM_SPEC] + [vmem_spec()] * 4,
        out_specs=[vmem_spec()] * 2,
        out_shape=[jax.ShapeDtypeStruct((2, rows + 2, count), f32)] * 2,
        compiler_params=params(0),
        cost_estimate=cost(300_000_000, 500_000),
        name="pack_sides",
    )(where, low, high, west, east)


def lane_cuts(count):
    return [slice(at, min(at + LANES, count)) for at in range(0, count, LANES)]


def advect_kernel(
    n_aa,
    where_ref,
    bins_ref,
    spectra_ref,
    mask_ref,
    low_ref,
    high_ref,
    west_ref,
    east_ref,
    out_ref,
    first,
    second,
    edges,
    masks,
    padded,
):
    rows, columns, bins = spectra_ref.shape
    half = where_ref[2]
    turned = transposed_mask(mask_ref, padded)

    def spread(column):
        return jnp.broadcast_to(column, (columns, LANES))

    low_far, high_far = rows_beyond(n_aa, where_ref, low_ref, high_ref, 0)
    low_near, high_near = rows_beyond(n_aa, where_ref, low_ref, high_ref, 1)
    first[0] = low_far[:, :bins]
    first[1] = low_near[:, :bins]
    first[rows + 2] = high_near[:, :bins]
    first[rows + 3] = high_far[:, :bins]
    masks[0] = spread(low_near[:, bins:])
    masks[rows + 1] = spread(high_near[:, bins:])
    for row in range(rows):
        own = spread(column_of(turned, row)[:columns])
        masks[row + 1] = own
        for cut in lane_cuts(bins):
            first[row + 2, :, cut] = spectra_ref[row, :, cut] * own[:, : cut.stop - cut.start]

    def update(cut, centre, western, eastern, southern, northern):
        keep, east_pos, east_neg, north_pos, north_neg = (
            bins_ref[half, at : at + 1, cut] for at in range(5)
        )
        return (
            keep * centre
            + east_pos * western
            + east_neg * eastern
            + north_pos * southern
            + north_neg * northern
        )

    beside = slice(1, rows + 1)
    for cut in lane_cuts(bins):
        near, far = west_ref[1, :, cut], west_ref[0, :, cut]
        inside = first[2 : rows + 2, 0, cut]
        edges[0, :, cut] = west_ref[1, beside, bins:] * update(
            cut, near[1 : rows + 1], far[1 : rows + 1], inside, near[:rows], near[2:]
        )
        near, far = east_ref[0, :, cut], east_ref[1, :, cut]
        inside = first[2 : rows + 2, columns - 1, cut]
        edges[1, :, cut] = east_ref[0, beside, bins:] * update(
            cut, near[1 : rows + 1], inside, far[1 : rows + 1], near[:rows], near[2:]
        )

    def step(source, at, cut, west_column, east_column):
        centre = source[at, :, cut]
        place = lax.broadcasted_iota(jnp.int32, centre.shape, 0)
        western = jnp.where(place == 0, west_column, pltpu.roll(centre, 1, 0))
        eastern = jnp.where(
            place == columns - 1, east_column, pltpu.roll(centre, columns - 1, 0)
        )
        return update(
            cut, centre, western, eastern, source[at - 1, :, cut], source[at + 1, :, cut]
        )

    for cut in lane_cuts(bins):
        size = cut.stop - cut.start
        for row in range(rows + 2):
            at = slice(row, row + 1)
            value = step(first, row + 1, cut, west_ref[1, at, cut], east_ref[0, at, cut])
            second[row, :, cut] = value * masks[row, :, :size]
    for cut in lane_cuts(bins):
        size = cut.stop - cut.start
        for row in range(rows):
            at = slice(row, row + 1)
            value = step(second, row + 1, cut, edges[0, at, cut], edges[1, at, cut])
            out_ref[row, :, cut] = value * masks[row + 1, :, :size]


def advect(where, bins, spectra, mask, low, high, west, east, n_aa):
    rows, columns, count = spectra.shape
    return pl.pallas_call(
        functools.partial(advect_kernel, n_aa),
        in_specs=[SMEM_SPEC] + [vmem_spec()] * 7,
        out_specs=vmem_spec(),
        out_shape=jax.ShapeDtypeStruct(spectra.shape, f32),
        scratch_shapes=[
            pltpu.VMEM((rows + 4, columns, count), f32),
            pltpu.VMEM((rows + 2, columns, count), f32),
            pltpu.VMEM((2, rows, count), f32),
            pltpu.VMEM((rows + 2, columns, LANES), f32),
            pltpu.VMEM((LANES, LANES), f32),
        ],
        compiler_params=params(0),
        cost_estimate=cost(2_600_000_000, 4_000_000),
        name="advect",
    )(where, bins, spectra, mask, low, high, west, east)


def across(sent, axis):
    count = lax.axis_size(axis)
    if len(sent) == 1:
        got = lax.ppermute(sent[0], axis, [(0, 1), (1, 0)])
        return got, got
    forward = [(i, i + 1) for i in range(count - 1)]
    backward = [(target, source) for source, target in forward]
    return lax.ppermute(sent[1], axis, forward), lax.ppermute(sent[0], axis, backward)


def as_columns(rows_by_lanes):
    rows = rows_by_lanes.shape[0]
    if rows % 8:
        rows_by_lanes = jnp.concatenate(
            [rows_by_lanes, jnp.zeros((8 - rows % 8, LANES), f32)], axis=0
        )
    return jnp.transpose(rows_by_lanes)


def stress_kernel(
    n_in, where_ref, bins_ref, density_ref, own_ref, own_far_ref, other_ref, other_far_ref,
    sums_ref, points_ref
):
    cycles = own_ref.shape[0]
    rows, _, bins = density_ref.shape
    cycle_rows = rows // cycles
    half = where_ref[2]
    holds = lax.rem(where_ref[1], n_in) == 0
    own = jnp.where(holds, own_ref[...], own_far_ref[...])
    other = jnp.where(holds, other_ref[...], other_far_ref[...])
    east_rows = jnp.where(half == 0, own, other)
    north_rows = jnp.where(half == 0, other, own)
    points_ref[0] = east_rows
    points_ref[1] = north_rows
    points_ref[2] = drag_coef * (own * own + other * other) + stress_floor
    east, north = as_columns(east_rows), as_columns(north_rows)
    along_cos, along_sin, width = (bins_ref[half, at : at + 1] for at in (5, 6, 7))
    lane = lax.broadcasted_iota(jnp.int32, (LANES, LANES), 1)
    sums = jnp.zeros((LANES, LANES), f32)
    for cycle in range(cycles):
        density = density_ref[cycle * cycle_rows : (cycle + 1) * cycle_rows].reshape(LANES, bins)
        alignment = (
            east[:, cycle : cycle + 1] * along_cos + north[:, cycle : cycle + 1] * along_sin
        )
        weighted = density * width
        gain = growth * jnp.maximum(alignment - 1.0, 0.0)
        energy = jnp.sum(weighted, axis=1, keepdims=True)
        stress = jnp.sum(gain * alignment * weighted, axis=1, keepdims=True)
        sums = jnp.where(lane == cycle, stress, sums)
        sums = jnp.where(lane == cycles + cycle, energy, sums)
    turned = jnp.transpose(sums)
    sums_ref[0] = turned[:cycles]
    sums_ref[1] = turned[cycles : 2 * cycles]


def stress_sums(where, bins, density, winds, n_in):
    cycles = winds[0].shape[0]
    return pl.pallas_call(
        functools.partial(stress_kernel, n_in),
        in_specs=[SMEM_SPEC] + [vmem_spec()] * 6,
        out_specs=[vmem_spec()] * 2,
        out_shape=[
            jax.ShapeDtypeStruct((2, cycles, LANES), f32),
            jax.ShapeDtypeStruct((3, cycles, LANES), f32),
        ],
        compiler_params=params(0),
        cost_estimate=cost(1_500_000_000, 2_000_000),
        name="stress",
    )(where, bins, density, *winds)


def spectra_kernel(
    where_ref, bins_ref, density_ref, points_ref, sums_ref, far_ref, out_hbm, value_ref, done
):
    half = where_ref[2]
    rows, columns, bins = density_ref.shape
    cycles = points_ref.shape[1]
    cycle_rows = rows // cycles
    scaled = (sums_ref[1] + far_ref[1]) * (1.0 / energy_ref)
    east, north = as_columns(points_ref[0]), as_columns(points_ref[1])
    energy = as_columns(scaled * scaled)
    along_cos, along_sin, decay = (bins_ref[half, at : at + 1] for at in (5, 6, 8))
    copies = []
    for cycle in range(cycles):
        at = slice(cycle * cycle_rows, (cycle + 1) * cycle_rows)
        own = slice(cycle, cycle + 1)
        density = density_ref[at].reshape(LANES, bins)
        alignment = east[:, own] * along_cos + north[:, own] * along_sin
        gain = growth * jnp.maximum(alignment - 1.0, 0.0)
        value = density * (1.0 + gain) / (1.0 + decay * energy[:, own])
        value_ref[at] = value.reshape(cycle_rows, columns, bins)
        copies.append(
            pltpu.make_async_copy(value_ref.at[at], out_hbm.at[at], done.at[cycle])
        )
        copies[-1].start()
    for copy in copies:
        copy.wait()


def final_spectra(where, bins, density, points, sums, far):
    cycles = points.shape[1]
    return pl.pallas_call(
        spectra_kernel,
        in_specs=[SMEM_SPEC] + [vmem_spec()] * 5,
        out_specs=pl.BlockSpec(memory_space=pltpu.HBM),
        out_shape=jax.ShapeDtypeStruct(density.shape, f32),
        scratch_shapes=[
            pltpu.VMEM(density.shape, f32),
            pltpu.SemaphoreType.DMA((cycles,)),
        ],
        compiler_params=params(0),
        cost_estimate=cost(2_500_000_000, 3_000_000),
        name="spectra",
    )(where, bins, density, points, sums, far)


def charnock_kernel(shape, where_ref, count_ref, source_ref, *refs):
    columns_local, total_columns, order = shape
    rough_refs, out_ref = refs[:-1], refs[-1]
    column = where_ref[1]
    cycles, width = source_ref.shape
    cycle_rows = LANES // columns_local
    base = column * width
    row = lax.broadcasted_iota(jnp.int32, (cycles, LANES), 0)
    points = jnp.zeros((cycles, LANES), jnp.int32)
    for cycle in range(cycles):
        points = jnp.where(row == cycle, count_ref[where_ref[0] * cycles + cycle], points)
    lane = lax.broadcasted_iota(jnp.int32, (cycles, LANES), 1)
    for part in range(width // LANES):
        at = slice(part * LANES, (part + 1) * LANES)
        source = source_ref[:, at]
        band_row = source // total_columns
        source_column = source - band_row * total_columns
        owner = source_column // columns_local
        within = (band_row - row * cycle_rows) * columns_local + (
            source_column - owner * columns_local
        )
        within = jnp.clip(within, 0, LANES - 1)
        value = jnp.zeros((cycles, LANES), f32)
        for rough_ref, distances in zip(rough_refs, order):
            for at_piece, distance in enumerate(distances):
                found = jnp.take_along_axis(rough_ref[at_piece], within, axis=1)
                value = jnp.where(owner == jnp.bitwise_xor(column, distance), found, value)
        out_ref[:, at] = jnp.where(lane + (base + part * LANES) < points, value, 0.0)


def charnock_of(where, counts, pieces, order, source, columns_local):
    total_columns = columns_local * sum(len(distances) for distances in order)
    return pl.pallas_call(
        functools.partial(charnock_kernel, (columns_local, total_columns, order)),
        in_specs=[SMEM_SPEC, SMEM_SPEC] + [vmem_spec()] * (1 + len(pieces)),
        out_specs=vmem_spec(),
        out_shape=jax.ShapeDtypeStruct(source.shape, f32),
        compiler_params=params(0),
        cost_estimate=cost(1_000_000_000, 100_000),
        name="charnock",
    )(where, counts, source, *pieces)


def exchange(value, axis, distance):
    count = lax.axis_size(axis)
    return lax.ppermute(value, axis, [(i, i ^ distance) for i in range(count)])


def exchange_both(value, n_comp, n_ba):
    pairs = [
        (half * n_ba + i, (half ^ 1) * n_ba + (i ^ 1))
        for half in range(n_comp)
        for i in range(n_ba)
    ]
    return lax.ppermute(value, ("comp", "ba"), pairs)


def per_device(
    legendre, coefficients, cycle_points, spectra, sea_mask, wind_column, roughness_source
):
    n_aa, n_ba = lax.axis_size("aa"), lax.axis_size("ba")
    n_comp = lax.axis_size("comp")
    band_index = lax.axis_index("aa")
    column_index = lax.axis_index("ba")
    half_index = lax.axis_index("comp")
    where = jnp.stack([band_index, column_index, half_index]).astype(jnp.int32)
    waves_local, cycles_all, _ = legendre.shape
    cycles = cycles_all // n_aa
    rows_local, columns_local, _ = spectra.shape
    cycle_rows = rows_local // cycles
    n_in = 2
    n_out = n_ba // n_in
    slots_local = LON // n_ba
    counts = cycle_points
    bins = jnp.asarray(bin_table(n_comp))

    fourier = legendre_sums(legendre, coefficients, where, n_aa)

    *row_sides, west, east = pack(where, spectra, sea_mask, n_aa)
    low, high = across(row_sides, "aa")
    west, east = pack_sides(where, low, high, west, east, n_aa)
    west, east = across([west, east], "ba")
    density = advect(where, bins, spectra, sea_mask, low, high, west, east, n_aa)
    wind_table = wind_tables(
        wind_column, counts, where, n_aa, waves_local, n_in,
        (cycles, cycle_rows, columns_local),
    )

    parts = [fourier[0]]
    for shift in range(1, n_aa):
        pairs = [(i, (i + shift) % n_aa) for i in range(n_aa)]
        parts.append(lax.ppermute(fourier[shift], "aa", pairs))
    parts = jnp.stack(parts)
    outer = [parts]
    for k in range(1, n_out):
        outer.append(exchange(parts, "ba", n_in * k))
    outer = jnp.stack(outer)

    picked = pick_winds(outer, wind_table, where, n_aa, waves_local, n_in)
    own_sent = exchange(picked[1], "ba", 1)
    other_sent = exchange_both(picked[1], n_comp, n_ba)
    other_here = exchange(picked[0], "comp", 1)
    inner = [outer]
    for k in range(1, n_in):
        inner.append(exchange(outer, "ba", k))

    winds = (picked[0], own_sent, other_here, other_sent)
    sums, points = stress_sums(where, bins, density, winds, n_in)
    far = exchange(sums, "comp", 1)
    roughness = jnp.sqrt(1.0 + stress_coef * (sums[0] + far[0]) / points[2])
    pieces, order = [roughness[None]], [(0,)]
    for distance in [n_in << k for k in range(n_out.bit_length() - 1)] + [1]:
        sent = jnp.concatenate(pieces, axis=0)
        pieces.append(exchange(sent, "ba", distance))
        order.append(tuple(far_at ^ distance for near in order for far_at in near))
    wave_spectra = final_spectra(where, bins, density, points, sums, far)
    grid_table = grid_tables(counts, where, cycles, n_aa, waves_local, slots_local)
    grid_winds = synthesis(inner, grid_table, where, n_aa, waves_local, n_in)
    grid_winds = grid_winds.reshape(1, cycles, -1, slots_local)
    charnock = charnock_of(
        where, counts, pieces, tuple(order), roughness_source, columns_local
    )
    return (grid_winds, wave_spectra, charnock)


def solution(mesh):
    in_specs = (
        P("aa", None, None),
        P("comp", "aa", None, "ba", None),
        P(),
        P("aa", "ba", "comp"),
        P("aa", "ba"),
        P("aa", None),
        P("aa", "ba"),
    )
    out_specs = (P("comp", "aa", None, "ba"), P("aa", "ba", "comp"), P("aa", "ba"))
    return jax.shard_map(
        per_device, mesh=mesh, in_specs=in_specs, out_specs=out_specs, check_vma=False
    )
```
